256 devices in a mesh: rep: 2 (over z), exp: 128 (over x, y, core).
Axes of the slice: x: 8, y: 8, z: 2, core: 2. Of those that a mesh axis runs over, the one named last changes fastest.
The devices are a block of a 8x8x16 slice.
Arguments:
- a_tokens: bfloat16 [512, 7168], P(('rep', 'exp')), parts along dimension 0, may hold values from -6 to 6
- a_gain: float32 [7168], replicated, may hold values from 0.25 to 1.75
- dense_gate: bfloat16 [7168, 18432], P(None, 'exp'), may hold values from -0.0625 to 0.0625
- dense_up: bfloat16 [7168, 18432], P(None, 'exp'), may hold values from -0.0625 to 0.0625
- dense_down: bfloat16 [18432, 7168], P('exp'), may hold values from -0.046875 to 0.046875
- b_tokens: bfloat16 [1024, 7168], P(('rep', 'exp')), parts along dimension 0, may hold values from -6 to 6
- b_gain: float32 [7168], replicated, may hold values from 0.25 to 1.75
- expert_ids: int32 [1024, 8], P(('rep', 'exp')), parts along dimension 0, may hold values from 0 to 15, all different within a row; in each aligned block of 4 rows (0 to 3, 4 to 7, ...) at most 3 rows name the same one
- route_weights: float32 [1024, 8], P(('rep', 'exp')), parts along dimension 0, may hold values from 0.05 to 0.5
- expert_gate: bfloat16 [128, 7168, 128], P('exp'), may hold values from -0.0625 to 0.0625
- expert_up: bfloat16 [128, 7168, 128], P('exp'), may hold values from -0.0625 to 0.0625
- expert_down: bfloat16 [128, 128, 7168], P('exp'), may hold values from -0.1875 to 0.1875
Outputs:
- a_out: bfloat16 [512, 7168], P(('rep', 'exp')), parts along dimension 0
- b_out: bfloat16 [1024, 7168], P(('rep', 'exp')), parts along dimension 0
The draws below stay inside these ranges and needn't reach their ends.
There are 2 independent parts, one for each index of `rep`. The reference program is written for one: setup_inputs(seed, part) draws one part's arguments, and reference() takes and returns one part's arrays. A program takes and returns all parts, laid end to end along the dimension named above; an argument that names none is the same for every part. Nothing has to cross between parts.
Inputs may be any that keep to these rules, and one draw needn't show every extreme that they name: `expert_ids`: each row names 8 different experts. Among the rows of one device no expert is named more than 3 times, and in some devices one expert is named exactly 3 times.
All inputs are finite; a program needn't handle non-finite values.
Results may differ from the reference program's by a relative error of at most 0.008.
Values may be sent and summed in bfloat16 or wider, within the bound.
No kernel may reach another device: no remote copies, remote signals or barrier semaphores. Data moves between devices by JAX's collectives and lax.ppermute only.
A program may use at most 128 MiB of HBM per device.

```python
import math
import jax
import jax.numpy as jnp
import numpy as np
from jax import lax

D = 7168
FF = 18432
EH = 1024
EXPERTS = 16
TOPK = 8
TB_DEV = 4
TA = 256
TB = 512
GROUP = 8
ES = 128
CAP = 3


def levels(stream_key, extent, pieces, low, high):
    def one(position, parts):
        draws = jax.random.uniform(jax.random.fold_in(jax.random.fold_in(stream_key, 6), position), (parts,), jnp.float32, low / len(pieces), high / len(pieces))
        return jnp.repeat(jnp.exp(draws), extent[position] // parts).reshape((-1,) + (1,) * (len(extent) - position - 1))

    level = one(*pieces[0])
    for cut in pieces[1:]:
        level = level * one(*cut)
    return level


def shared_out(stream_key, own, number, rows, amount, top, bound, slope):
    order = jax.random.permutation(stream_key, amount)
    packed, ordinary = load_shares(amount, rows * top, bound, slope, True), load_shares(amount, rows * top, bound, slope, False)
    places = jnp.arange(amount)

    def named(sizes, offset_by):
        used = int((sizes > 0).sum())
        fixed = max(1, used // 4)
        shifted = fixed + (places - fixed + offset_by * (used - fixed)) % max(1, amount - fixed)
        return jnp.zeros((amount,), jnp.int32).at[order[jnp.where(places < fixed, places, shifted)]].set(jnp.asarray(sizes, jnp.int32))

    sizes = jnp.where(number % 4 == 0, named(packed, number // 4), named(ordinary, number - number // 4 - 1))
    mixed = jax.random.permutation(jax.random.fold_in(own, 3), amount)
    donor, receiver = mixed[0:amount // 2 * 2:2], mixed[1:amount // 2 * 2:2]
    slack = jnp.minimum(sizes[donor] - 1, bound - sizes[receiver]) // 2
    slack = jnp.where((donor == order[0]) | (receiver == order[0]) | (sizes[receiver] == 0), 0, jnp.maximum(slack, 0))
    shifted = jax.random.randint(jax.random.fold_in(own, 4), (amount // 2,), 0, 1 << 20) % (slack + 1)
    sizes = sizes.at[donor].add(-shifted).at[receiver].add(shifted)
    labels = jnp.searchsorted(jnp.cumsum(sizes), jnp.arange(rows * top), side="right").astype(jnp.int32)
    table = labels.reshape(top, rows).T
    table = table[jax.random.permutation(jax.random.fold_in(own, 1), rows)]
    offset_by = jax.random.randint(jax.random.fold_in(own, 2), (rows, 1), 0, top)
    return jnp.take_along_axis(table, (jnp.arange(top)[None, :] + offset_by) % top, axis=1)


def load_shares(amount, total, reach, skew, full):
    portions = [(1 << 20) // math.isqrt(grade ** skew) + 1 for grade in range(1, amount + 1)]
    largest = reach if full else min(reach, max(-(-total // amount), total * portions[0] // sum(portions)))
    least = 1 if total - largest >= amount - 1 else 0
    counts, spare = [largest] + [least] * (amount - 1), total - largest - least * (amount - 1)
    while spare > 0:
        candidates = [i for i in range(1, amount) if counts[i] < largest] or [i for i in range(1, amount) if counts[i] < reach]
        whole, left = sum([portions[i] for i in candidates]), spare
        for i in candidates:
            more = min(reach - counts[i], max(1, left * portions[i] // whole), spare)
            counts[i] = counts[i] + more
            spare = spare - more
    return np.array(counts)


def noise(stream_key, shape, scale, most, cuts=(), kind=jnp.bfloat16):
    values = jax.random.normal(stream_key, shape, jnp.float32) * scale
    if len(cuts) > 0:
        values = levels(stream_key, shape, cuts, -0.22, 0.18) * values
    return jnp.clip(values, min=-most, max=most).astype(kind)


def setup_inputs(seed: int = 0, part: int = 0) -> dict:
    splits = jax.random.split(jax.random.key(seed), 13)
    own_keys = jax.random.split(jax.random.fold_in(splits[12], part), 13)
    a_tokens = noise(own_keys[0], (TA, D), 1.0, 6.0, ((0, 128),))
    a_gain = jnp.clip(1.0 + 0.15 * jax.random.normal(splits[1], (D,), jnp.float32), 0.25, 1.75)
    dense_gate = noise(splits[2], (D, FF), D ** -0.5, 0.0625, ((1, 128),))
    dense_up = noise(splits[3], (D, FF), D ** -0.5, 0.0625, ((1, 128),))
    dense_down = noise(splits[4], (FF, D), FF ** -0.5, 0.046875, ((0, 128),))
    b_tokens = noise(own_keys[5], (TB, D), 1.0, 6.0, ((0, 128),))
    b_gain = jnp.clip(1.0 + 0.15 * jax.random.normal(splits[6], (D,), jnp.float32), 0.25, 1.75)
    expert_ids_keys = jax.random.split(jax.random.fold_in(own_keys[7], 1), TB // TB_DEV)
    expert_ids_turns = jax.random.permutation(jax.random.fold_in(own_keys[7], 3), TB // TB_DEV)
    expert_ids = jax.vmap(lambda own, number: shared_out(jax.random.fold_in(own_keys[7], 2), own, number, TB_DEV, EXPERTS, TOPK, CAP, 2))(expert_ids_keys, expert_ids_turns).reshape((TB, TOPK))
    route_weights = jnp.clip(jnp.exp(math.log(0.5) - 2.3025851 * jax.random.uniform(own_keys[8], (TB, TOPK), jnp.float32) ** levels(own_keys[8], (TB, TOPK), ((0, 128),), -0.2, 0.2)), 0.05, 0.5)
    expert_gate = noise(splits[9], (EXPERTS * GROUP, D, ES), D ** -0.5, 0.0625, ((0, 128),))
    expert_up = noise(splits[10], (EXPERTS * GROUP, D, ES), D ** -0.5, 0.0625, ((0, 128),))
    expert_down = noise(splits[11], (EXPERTS * GROUP, ES, D), EH ** -0.5, 0.1875, ((0, 128),))
    return dict(a_tokens=a_tokens, a_gain=a_gain, dense_gate=dense_gate, dense_up=dense_up, dense_down=dense_down, b_tokens=b_tokens, b_gain=b_gain, expert_ids=expert_ids, route_weights=route_weights, expert_gate=expert_gate, expert_up=expert_up, expert_down=expert_down)


def normed(values, gain_vec):
    return values * lax.rsqrt(lax.optimization_barrier(jnp.mean(values * values, axis=-1, keepdims=True)) + 1e-06) * gain_vec

def reference(a_tokens, a_gain, dense_gate, dense_up, dense_down, b_tokens, b_gain, expert_ids, route_weights, expert_gate, expert_up, expert_down):
    a_float = a_tokens.astype(jnp.float32)
    a_normed = normed(a_float, a_gain).astype(jnp.bfloat16)
    gate_proj = jnp.dot(a_normed, dense_gate, preferred_element_type=jnp.float32)
    up_proj = jnp.dot(a_normed, dense_up, preferred_element_type=jnp.float32)
    hidden = (jax.nn.silu(gate_proj) * up_proj).astype(jnp.bfloat16)
    a_out = (a_float + jnp.dot(hidden, dense_down, preferred_element_type=jnp.float32)).astype(jnp.bfloat16)
    b_float = b_tokens.astype(jnp.float32)
    b_normed = normed(b_float, b_gain).astype(jnp.bfloat16)
    b_wide = b_normed.astype(jnp.float32)
    onehot = (expert_ids[:, :, None] == jnp.arange(EXPERTS, dtype=jnp.int32)[None, None, :]).astype(jnp.float32)
    mix_table = jnp.einsum('tk,tke->et', route_weights.astype(jnp.float32), onehot)
    gate_blocks = expert_gate.reshape(EXPERTS, GROUP, D, ES)
    up_blocks = expert_up.reshape(EXPERTS, GROUP, D, ES)
    down_blocks = expert_down.reshape(EXPERTS, GROUP, ES, D)

    def one_expert(running, inputs):
        w_gate, w_up, w_down, weight = inputs
        gate_e = jnp.einsum('td,gds->tgs', b_wide, w_gate.astype(jnp.float32))
        up_e = jnp.einsum('td,gds->tgs', b_wide, w_up.astype(jnp.float32))
        hid_e = (jax.nn.silu(gate_e) * up_e).astype(jnp.bfloat16)
        partial_value = jnp.einsum('tgs,gsd->tgd', hid_e.astype(jnp.float32), w_down.astype(jnp.float32)).astype(jnp.bfloat16)
        expert_out = lax.optimization_barrier(jnp.sum(partial_value.astype(jnp.float32), axis=1)).astype(jnp.bfloat16)
        return (running + weight[:, None] * expert_out.astype(jnp.float32), None)
    totals, _ = lax.scan(one_expert, jnp.zeros((TB, D), jnp.float32), (gate_blocks, up_blocks, down_blocks, mix_table))
    b_out = (b_float + totals).astype(jnp.bfloat16)
    return (a_out, b_out)
```

```python
import jax
import jax.numpy as jnp
from jax import lax
from jax.experimental import pallas as pl
from jax.experimental.pallas import tpu as pltpu
from jax.sharding import Mesh
from jax.sharding import PartitionSpec as P

EXPERTS = 16
RING = 8
CORES = 2
EXP = ("exp_0", "exp_1", "exp_2")
REP_EXP = ("rep", "exp_0", "exp_1", "exp_2")


def pairs_along(stage, distance):
    pairs = []
    for x in range(RING):
        for y in range(RING):
            for c in range(CORES):
                along_x = (stage == 2) == (c == 0)
                to_x = (x + distance) % RING if along_x else x
                to_y = y if along_x else (y + distance) % RING
                pairs.append(((x * RING + y) * CORES + c, (to_x * RING + to_y) * CORES + c))
    return pairs


def move(array, stage, distance):
    return lax.ppermute(array, EXP, pairs_along(stage, distance))


def swap_cores(array):
    devices = RING * RING * CORES
    return lax.ppermute(array, EXP, [(i, i ^ 1) for i in range(devices)])


def normed(values, gain_vec):
    return values * lax.rsqrt(jnp.mean(values * values, axis=-1, keepdims=True) + 1e-06) * gain_vec


ORDER = (4, 3, -3, 2, -2, 1, -1, 0)


def stage_1_groups():
    first = [[(x * RING + y) * CORES for y in range(RING)] for x in range(RING)]
    second = [[(x * RING + y) * CORES + 1 for x in range(RING)] for y in range(RING)]
    return first + second


def exchange(blocks):
    return lax.all_to_all(
        blocks, EXP, split_axis=0, concat_axis=0, tiled=True, axis_index_groups=stage_1_groups()
    )


def gather_ring(block, cut):
    slots = {0: block}
    for k in (1, 2, 3):
        slots[k] = move(slots[k - 1], 2, 1)
        slots[-k] = move(slots[1 - k], 2, -1)
    far_low = move(slots[3][:, :cut], 2, 1)
    far_high = move(slots[-3][:, cut:], 2, -1)
    return [far_low, far_high] + [slots[k] for k in ORDER[1:]]


def scatter_ring(own, other_far, other_near):
    rows = own.shape[0] // RING
    cut = own.shape[1] // 2
    far_rows = other_far.shape[0]

    def part(k):
        at = ORDER.index(k) * rows
        other = other_far[at : at + rows] if at < far_rows else other_near[at - far_rows :][:rows]
        return own[at : at + rows].astype(jnp.float32) + other.astype(jnp.float32)

    far = part(4).astype(jnp.bfloat16)
    low = move(far[:, :cut], 2, -1).astype(jnp.float32)
    high = move(far[:, cut:], 2, 1).astype(jnp.float32)
    down = jnp.concatenate([part(3)[:, :cut] + low, part(3)[:, cut:]], 1)
    up = jnp.concatenate([part(-3)[:, :cut], part(-3)[:, cut:] + high], 1)
    for k in (2, 1, 0):
        down = move(down.astype(jnp.bfloat16), 2, -1).astype(jnp.float32)
        up = move(up.astype(jnp.bfloat16), 2, 1).astype(jnp.float32)
        if k:
            down = part(k) + down
            up = part(-k) + up
    return part(0) + down + up


def layer_kernel(blocks, gate, up, down, pick, cut, name):
    rows = blocks[2].shape[0]
    full = blocks[2].shape[1]
    width = down.shape[1]
    hidden = down.shape[0]
    count = 2 * RING
    total = count * rows
    flip = gate.shape[1] == width
    per = RING + 1
    chunk = 1024
    far = 3 * rows
    inputs = list(blocks) + [gate, up, down] + ([] if pick is None else [pick])
    n_in = len(inputs)

    def body(*refs):
        ins = refs[:n_in]
        own_ref, far_ref, near_ref = refs[n_in : n_in + 3]
        x, wg, wu, wd, acc_g, acc_u, hid, sems, wsems = refs[n_in + 3 :]
        copies = []
        for i in range(2 * per):
            core, j = divmod(i, per)
            slot = core * RING + max(j - 1, 0)
            at = pl.ds(slot * rows, rows)
            if j == 0:
                to = x.at[at, pl.ds(0, cut)]
            elif j == 1:
                to = x.at[at, pl.ds(cut, full - cut)]
            else:
                to = x.at[at, :]
            copies.append(pltpu.make_async_copy(ins[i], to, sems.at[i]))
        weights = [
            pltpu.make_async_copy(ins[2 * per + i], to, wsems.at[i])
            for i, to in enumerate((wg, wu, wd))
        ]
        for c in weights + copies:
            c.start()
        weights[0].wait()
        weights[1].wait()
        for c in copies:
            c.wait()
        acc_g[...] = jnp.zeros_like(acc_g)
        acc_u[...] = jnp.zeros_like(acc_u)

        def step(i, carry):
            at = pl.ds(pl.multiple_of(i * chunk, chunk), chunk)
            part = x[:, at]
            for acc, w in ((acc_g, wg), (acc_u, wu)):
                if flip:
                    acc[...] += lax.dot_general(
                        part, w[:, at], (((1,), (1,)), ((), ())), preferred_element_type=jnp.float32
                    )
                else:
                    acc[...] += jnp.dot(part, w[at, :], preferred_element_type=jnp.float32)
            return carry

        lax.fori_loop(0, width // chunk, step, 0)
        g = acc_g[...]
        value = g * (1.0 / (1.0 + jnp.exp(-g))) * acc_u[...]
        if pick is not None:
            tail = x[:, width:].astype(jnp.float32) * ins[n_in - 1][...]
            value = value * jnp.sum(tail, axis=1, keepdims=True)
        hid[...] = value.astype(jnp.bfloat16)
        weights[2].wait()

        def out_step(i, carry):
            at = pl.ds(pl.multiple_of(i * chunk, chunk), chunk)
            w = wd[:, at]
            half = RING * rows
            for ref, lo, n in ((far_ref, half, far), (near_ref, half + far, half - far), (own_ref, 0, half)):
                ref[:, at] = jnp.dot(
                    hid[lo : lo + n, :], w, preferred_element_type=jnp.float32
                ).astype(jnp.bfloat16)
            return carry

        lax.fori_loop(0, width // chunk, out_step, 0)

    any_spec = pl.BlockSpec(memory_space=pl.ANY)
    specs = [any_spec] * (n_in if pick is None else n_in - 1)
    if pick is not None:
        specs.append(pl.BlockSpec(memory_space=pltpu.VMEM))
    half = RING * rows
    return pl.pallas_call(
        body,
        in_specs=specs,
        out_specs=[pl.BlockSpec(memory_space=pltpu.VMEM)] * 3,
        out_shape=[
            jax.ShapeDtypeStruct((half, width), jnp.bfloat16),
            jax.ShapeDtypeStruct((far, width), jnp.bfloat16),
            jax.ShapeDtypeStruct((half - far, width), jnp.bfloat16),
        ],
        scratch_shapes=[
            pltpu.VMEM((total, full), jnp.bfloat16),
            pltpu.VMEM(gate.shape, jnp.bfloat16),
            pltpu.VMEM(up.shape, jnp.bfloat16),
            pltpu.VMEM(down.shape, jnp.bfloat16),
            pltpu.VMEM((total, hidden), jnp.float32),
            pltpu.VMEM((total, hidden), jnp.float32),
            pltpu.VMEM((total, hidden), jnp.bfloat16),
            pltpu.SemaphoreType.DMA((2 * per,)),
            pltpu.SemaphoreType.DMA((3,)),
        ],
        cost_estimate=pl.CostEstimate(
            flops=6 * total * width * hidden,
            bytes_accessed=3 * width * hidden * 2 + total * full * 4,
            transcendentals=total * hidden,
        ),
        compiler_params=pltpu.CompilerParams(vmem_limit_bytes=48 * 1024 * 1024),
        name=name,
    )(*inputs)


def shards(
    a_tokens,
    a_gain,
    dense_gate,
    dense_up,
    dense_down,
    b_tokens,
    b_gain,
    expert_ids,
    route_weights,
    expert_gate,
    expert_up,
    expert_down,
):
    devices = lax.axis_size(EXP)
    group_size = devices // EXPERTS
    width = b_tokens.shape[1]
    a_rows = a_tokens.shape[0]
    b_rows = b_tokens.shape[0]
    a_float = a_tokens.astype(jnp.float32)
    a_normed = normed(a_float, a_gain).astype(jnp.bfloat16)
    b_float = b_tokens.astype(jnp.float32)
    b_normed = normed(b_float, b_gain).astype(jnp.bfloat16)
    onehot = (expert_ids[:, :, None] == jnp.arange(EXPERTS, dtype=jnp.int32)[None, None, :]).astype(
        jnp.float32
    )
    weights_te = jnp.sum(route_weights[:, :, None] * onehot, axis=1)
    first = lax.reduce_precision(weights_te, 8, 7)
    second = lax.reduce_precision(weights_te - first, 8, 7)
    third = weights_te - first - second
    extra = jnp.concatenate(
        [first, second, third, jnp.zeros((b_rows, 128 - 3 * EXPERTS), jnp.float32)], 1
    ).astype(jnp.bfloat16)
    wide = jnp.concatenate([b_normed, extra], 1)
    full = wide.shape[1]
    both = jnp.concatenate([jnp.pad(a_normed, ((0, 0), (0, full - width))), wide], 0)
    near = exchange(jnp.broadcast_to(both[None], (RING, *both.shape)))
    a_block = near[:, :a_rows, :width].reshape(RING * a_rows, width)
    b_block = near[:, a_rows:].reshape(RING * b_rows, full)

    cut = width // 2
    a_slots = gather_ring(a_block, cut)
    b_slots = gather_ring(b_block, cut)
    a_blocks = a_slots + [swap_cores(s) for s in a_slots]
    b_blocks = b_slots + [swap_cores(s) for s in b_slots]

    a_own, a_far, a_near = layer_kernel(
        a_blocks, dense_gate.T, dense_up.T, dense_down, None, cut, "dense_layer"
    )
    a_sum = scatter_ring(a_own, swap_cores(a_far), swap_cores(a_near))

    expert = lax.axis_index(EXP) // group_size
    lanes = jnp.arange(full - width)
    pick = ((lanes % EXPERTS == expert) & (lanes < 3 * EXPERTS)).astype(jnp.float32)[None, :]
    b_own, b_far, b_near = layer_kernel(
        b_blocks, expert_gate[0], expert_up[0], expert_down[0], pick, cut, "expert_layer"
    )
    b_sum = scatter_ring(b_own, swap_cores(b_far), swap_cores(b_near))

    both_sum = jnp.concatenate(
        [a_sum.reshape(RING, a_rows, width), b_sum.reshape(RING, b_rows, width)], 1
    )
    back = exchange(both_sum.astype(jnp.bfloat16)).astype(jnp.float32)
    total = jnp.sum(back, axis=0)
    a_out = (a_float + total[:a_rows]).astype(jnp.bfloat16)
    b_out = (b_float + total[a_rows:]).astype(jnp.bfloat16)
    return (a_out, b_out)


def solution(mesh):
    finer = Mesh(
        mesh.devices.reshape(mesh.shape["rep"], RING, RING, CORES),
        ("rep", "exp_0", "exp_1", "exp_2"),
    )
    placed = (
        P(REP_EXP, None),
        P(),
        P(None, EXP),
        P(None, EXP),
        P(EXP, None),
        P(REP_EXP, None),
        P(),
        P(REP_EXP, None),
        P(REP_EXP, None),
        P(EXP, None, None),
        P(EXP, None, None),
        P(EXP, None, None),
    )
    return jax.shard_map(
        shards,
        mesh=finer,
        in_specs=placed,
        out_specs=(P(REP_EXP, None), P(REP_EXP, None)),
        check_vma=False,
    )
```

```python
import jax
import jax.numpy as jnp
from jax import lax
from jax.experimental import pallas as pl
from jax.experimental.pallas import tpu as pltpu
from jax.sharding import Mesh
from jax.sharding import PartitionSpec as P


EXPERTS = 16
RING = 8
CORES = 2
EXP = ("exp_0", "exp_1", "exp_2")
REP_EXP = ("rep", "exp_0", "exp_1", "exp_2")


def pairs_along(stage, partner):
    pairs = []
    for x in range(RING):
        for y in range(RING):
            for c in range(CORES):
                along_x = (stage == 2) == (c == 0)
                to_x = partner(x) if along_x else x
                to_y = y if along_x else partner(y)
                pairs.append(((x * RING + y) * CORES + c, (to_x * RING + to_y) * CORES + c))
    return pairs


def even_partner(i):
    return i ^ 1


def odd_partner(i):
    return (((i + 1) % RING) ^ 1) - 1 if i else RING - 1


def over_even(array):
    return lax.ppermute(array, EXP, pairs_along(2, even_partner))


def over_odd(array):
    return lax.ppermute(array, EXP, pairs_along(2, odd_partner))


def swap_cores(array):
    devices = RING * RING * CORES
    return lax.ppermute(array, EXP, [(i, i ^ 1) for i in range(devices)])


def normed(values, gain_vec):
    return values * lax.rsqrt(jnp.mean(values * values, axis=-1, keepdims=True) + 1e-06) * gain_vec


GROUPS = ((0,), (1, -1), (2, -2), (3, -3, 4))


def stage_1_groups():
    first = [[(x * RING + y) * CORES for y in range(RING)] for x in range(RING)]
    second = [[(x * RING + y) * CORES + 1 for x in range(RING)] for y in range(RING)]
    return first + second


def exchange(blocks):
    return lax.all_to_all(
        blocks, EXP, split_axis=0, concat_axis=0, tiled=True, axis_index_groups=stage_1_groups()
    )


def gather_ring(block, cut):
    slots = {0: block}
    for k in (1, 2, 3):
        slots[k] = over_even(slots[1 - k])
        slots[-k] = over_odd(slots[k - 1])
    slots[4] = (over_even(slots[-3][:, :cut]), over_odd(slots[3][:, cut:]))
    return slots


def scatter_ring(own, other, streams):
    count = len(streams) - 1
    cuts = [(hi - lo) // 2 for lo, hi in zip(streams, streams[1:])]

    def part(k, i):
        at = slice(streams[i], streams[i + 1])
        return own[k][:, at].astype(jnp.float32) + other[k][:, at].astype(jnp.float32)

    low, high = [None] * count, [None] * count
    for i in range(count):
        far = part(4, i).astype(jnp.bfloat16)
        low[i] = over_even(far[:, : cuts[i]])
        high[i] = over_odd(far[:, cuts[i] :])
    for i in range(count):
        first, second = low[i].astype(jnp.float32), high[i].astype(jnp.float32)
        low[i] = jnp.concatenate([part(-3, i)[:, : cuts[i]] + first, part(-3, i)[:, cuts[i] :]], 1)
        high[i] = jnp.concatenate([part(3, i)[:, : cuts[i]], part(3, i)[:, cuts[i] :] + second], 1)
    for k in (2, 1, 0):
        for i in range(count):
            one, two = low[i].astype(jnp.bfloat16), high[i].astype(jnp.bfloat16)
            one = over_even(one) if k == 1 else over_odd(one)
            two = over_odd(two) if k == 1 else over_even(two)
            low[i], high[i] = one.astype(jnp.float32), two.astype(jnp.float32)
        if k:
            side = 1 if k == 2 else -1
            for i in range(count):
                low[i] = part(side * k, i) + low[i]
                high[i] = part(-side * k, i) + high[i]
    return jnp.concatenate([part(0, i) + low[i] + high[i] for i in range(count)], 1)


def layers(own, other, a_count, weights, pick, cut):
    units = pick.shape[1]
    width, dense_units = weights[2].shape[1], weights[2].shape[0]
    extra = dense_units - units
    full = width + units
    parts = []
    slots = 0
    for block in own + other:
        if isinstance(block, tuple):
            parts += [(block[0], slots, 0, cut), (block[1], slots, cut, None)]
        else:
            parts.append((block, slots, 0, None))
        slots += 1
    rows = parts[0][0].shape[0]
    b_count = rows - a_count
    half = slots // 2
    n_blocks = len(parts)
    inputs = [p[0] for p in parts] + list(weights) + [pick]
    n_in = len(inputs)
    chunk = 1024

    def body(*refs):
        ins = refs[:n_in]
        own_ref, other_ref = refs[n_in : n_in + 2]
        gate, up, da, e_gate, e_up, db = ins[n_blocks : n_blocks + 6]
        xa, xb, a_acc, b_acc, ha, hb, sems = refs[n_in + 2 :]
        a_copies, b_copies = [], []
        for i, (_, slot, lo, hi) in enumerate(parts):
            a_cols = pl.ds(lo, (width if hi is None else hi) - lo)
            b_cols = pl.ds(lo, (full if hi is None else hi) - lo)
            from_a = ins[i].at[pl.ds(0, a_count), pl.ds(0, a_cols.size)]
            from_b = ins[i].at[pl.ds(a_count, b_count), :]
            a_copies.append(
                pltpu.make_async_copy(from_a, xa.at[pl.ds(slot * a_count, a_count), a_cols], sems.at[2 * i])
            )
            b_copies.append(
                pltpu.make_async_copy(from_b, xb.at[pl.ds(slot * b_count, b_count), b_cols], sems.at[2 * i + 1])
            )
        for c in b_copies + a_copies:
            c.start()
        a_acc[...] = jnp.zeros_like(a_acc)
        b_acc[...] = jnp.zeros_like(b_acc)
        for c in b_copies:
            c.wait()

        def b_step(i, carry):
            at = pl.ds(pl.multiple_of(i * chunk, chunk), chunk)
            w = jnp.concatenate([e_gate[at, :], e_up[at, :]], 1)
            b_acc[...] += jnp.dot(xb[:, at], w, preferred_element_type=jnp.float32)
            return carry

        lax.fori_loop(0, width // chunk, b_step, 0)
        g = b_acc[:, :units]
        value = g * (1.0 / (1.0 + jnp.exp(-g))) * b_acc[:, units:]
        tail = xb[:, width:].astype(jnp.float32) * ins[n_in - 1][...]
        hb[...] = (value * jnp.sum(tail, axis=1, keepdims=True)).astype(jnp.bfloat16)
        for c in a_copies:
            c.wait()

        def a_step(i, carry):
            at = pl.ds(pl.multiple_of(i * chunk, chunk), chunk)
            w = jnp.concatenate([gate[:units, at], up[:units, at], gate[units:, at], up[units:, at]], 0)
            a_acc[...] += lax.dot_general(
                xa[:, at], w, (((1,), (1,)), ((), ())), preferred_element_type=jnp.float32
            )
            return carry

        lax.fori_loop(0, width // chunk, a_step, 0)
        for lo, n, to in ((0, units, 0), (2 * units, extra, units)):
            g = a_acc[:, lo : lo + n]
            u = a_acc[:, lo + n : lo + 2 * n]
            ha[:, to : to + n] = (g * (1.0 / (1.0 + jnp.exp(-g))) * u).astype(jnp.bfloat16)

        def out_step(i, carry):
            at = pl.ds(pl.multiple_of(i * chunk, chunk), chunk)
            for lo, count, h, w in ((0, a_count, ha, da), (a_count, b_count, hb, db)):
                r = jnp.dot(h[...], w[:, at], preferred_element_type=jnp.float32).astype(jnp.bfloat16)
                for slot in range(slots):
                    ref = own_ref if slot < half else other_ref
                    to = pl.ds(slot % half * rows + lo, count)
                    ref[to, at] = r[slot * count : (slot + 1) * count]
            return carry

        lax.fori_loop(0, width // chunk, out_step, 0)

    hbm_spec = pl.BlockSpec(memory_space=pltpu.HBM)
    vmem_spec = pl.BlockSpec(memory_space=pltpu.VMEM)
    a_total, b_total = slots * a_count, slots * b_count
    scratch = [
        ((a_total, width), jnp.bfloat16),
        ((b_total, full), jnp.bfloat16),
        ((a_total, 2 * dense_units), jnp.float32),
        ((b_total, 2 * units), jnp.float32),
        ((a_total, dense_units), jnp.bfloat16),
        ((b_total, units), jnp.bfloat16),
    ]
    return pl.pallas_call(
        body,
        in_specs=[hbm_spec] * n_blocks + [vmem_spec] * 7,
        out_specs=[vmem_spec] * 2,
        out_shape=[jax.ShapeDtypeStruct((half * rows, width), jnp.bfloat16)] * 2,
        scratch_shapes=[pltpu.VMEM(*s) for s in scratch]
        + [pltpu.SemaphoreType.DMA((2 * n_blocks,))],
        cost_estimate=pl.CostEstimate(
            flops=6 * width * (a_total * dense_units + b_total * units),
            bytes_accessed=6 * (dense_units + units) * width + 4 * (a_total + b_total) * width,
            transcendentals=0,
        ),
        compiler_params=pltpu.CompilerParams(vmem_limit_bytes=14 * 1024 * 1024),
    )(*inputs)


def prepare(a_tokens, a_gain, b_tokens, b_gain, expert_ids, route_weights):
    a_rows, width = a_tokens.shape
    rows = a_rows + b_tokens.shape[0]
    lanes = 128
    full = width + lanes

    def body(a_ref, ag_ref, b_ref, bg_ref, id_ref, w_ref, out_ref, hold):
        hold[:a_rows, :width] = normed(a_ref[...].astype(jnp.float32), ag_ref[...])
        hold[:a_rows, width:] = jnp.zeros((a_rows, lanes), jnp.float32)
        hold[a_rows:rows, :width] = normed(b_ref[...].astype(jnp.float32), bg_ref[...])
        lane = lax.broadcasted_iota(jnp.int32, (rows - a_rows, lanes), 1)
        expert = lane & (EXPERTS - 1)
        weight = jnp.zeros((rows - a_rows, lanes), jnp.float32)
        for k in range(expert_ids.shape[1]):
            weight += jnp.where(id_ref[:, k : k + 1] == expert, w_ref[:, k : k + 1], 0.0)
        first = weight.astype(jnp.bfloat16).astype(jnp.float32)
        second = (weight - first).astype(jnp.bfloat16).astype(jnp.float32)
        third = weight - first - second
        part = jnp.where(lane < EXPERTS, first, jnp.where(lane < 2 * EXPERTS, second, third))
        hold[a_rows:rows, width:] = jnp.where(lane < 3 * EXPERTS, part, 0.0)
        value = hold[:rows, :].astype(jnp.bfloat16)
        for i in range(RING):
            out_ref[i] = value

    vmem_spec = pl.BlockSpec(memory_space=pltpu.VMEM)
    return pl.pallas_call(
        body,
        in_specs=[vmem_spec] * 6,
        out_specs=vmem_spec,
        out_shape=jax.ShapeDtypeStruct((RING, rows, full), jnp.bfloat16),
        scratch_shapes=[pltpu.VMEM((8, full), jnp.float32)],
        cost_estimate=pl.CostEstimate(flops=20_000_000_000, bytes_accessed=1_000_000, transcendentals=0),
        compiler_params=pltpu.CompilerParams(vmem_limit_bytes=4 * 1024 * 1024),
        name="prepare",
    )(a_tokens, a_gain[None], b_tokens, b_gain[None], expert_ids, route_weights)


def pack(near, a_rows):
    places, rows, full = near.shape
    b_rows = rows - a_rows

    def body(near_ref, out_ref, hold):
        for i in range(places):
            value = near_ref[i].astype(jnp.float32)
            hold[pl.ds(i * a_rows, a_rows), :] = value[:a_rows]
            hold[pl.ds(places * a_rows + i * b_rows, b_rows), :] = value[a_rows:]
        out_ref[...] = hold[...].astype(jnp.bfloat16)

    vmem_spec = pl.BlockSpec(memory_space=pltpu.VMEM)
    return pl.pallas_call(
        body,
        in_specs=[vmem_spec],
        out_specs=vmem_spec,
        out_shape=jax.ShapeDtypeStruct((places * rows, full), jnp.bfloat16),
        scratch_shapes=[pltpu.VMEM((places * rows, full), jnp.float32)],
        compiler_params=pltpu.CompilerParams(vmem_limit_bytes=6 * 1024 * 1024),
        name="pack",
    )(near)


def shards(
    a_tokens,
    a_gain,
    dense_gate,
    dense_up,
    dense_down,
    b_tokens,
    b_gain,
    expert_ids,
    route_weights,
    expert_gate,
    expert_up,
    expert_down,
):
    devices = lax.axis_size(EXP)
    group_size = devices // EXPERTS
    width = b_tokens.shape[1]
    a_rows = a_tokens.shape[0]
    b_rows = b_tokens.shape[0]
    a_float = a_tokens.astype(jnp.float32)
    b_float = b_tokens.astype(jnp.float32)
    ready = prepare(a_tokens, a_gain, b_tokens, b_gain, expert_ids, route_weights)
    full = ready.shape[2]
    block = pack(exchange(ready), a_rows)
    cut = width // 2
    slots = gather_ring(block, cut)
    swapped = {
        k: tuple(swap_cores(p) for p in s) if isinstance(s, tuple) else swap_cores(s)
        for k, s in slots.items()
    }
    expert = lax.axis_index(EXP) // group_size
    lanes = jnp.arange(full - width)
    pick = ((lanes % EXPERTS == expert) & (lanes < 3 * EXPERTS)).astype(jnp.float32)[None, :]
    weights = (
        dense_gate.T,
        dense_up.T,
        dense_down,
        expert_gate[0],
        expert_up[0],
        expert_down[0],
    )
    own, other = {}, {}
    rows = block.shape[0]
    for group in GROUPS:
        mine, theirs = layers(
            [slots[k] for k in group],
            [swapped[k] for k in group],
            RING * a_rows,
            weights,
            pick,
            cut,
        )
        theirs = swap_cores(theirs)
        for i, k in enumerate(group):
            own[k] = mine[i * rows : (i + 1) * rows]
            other[k] = theirs[i * rows : (i + 1) * rows]
    streams = (0, width * 3 // 7, width)
    total = scatter_ring(own, other, streams)
    both_sum = jnp.concatenate(
        [
            total[: RING * a_rows].reshape(RING, a_rows, width),
            total[RING * a_rows :].reshape(RING, b_rows, width),
        ],
        1,
    )
    back = exchange(both_sum.astype(jnp.bfloat16)).astype(jnp.float32)
    total = jnp.sum(back, axis=0)
    a_out = (a_float + total[:a_rows]).astype(jnp.bfloat16)
    b_out = (b_float + total[a_rows:]).astype(jnp.bfloat16)
    return (a_out, b_out)


def solution(mesh):
    finer = Mesh(
        mesh.devices.reshape(mesh.shape["rep"], RING, RING, CORES),
        ("rep", "exp_0", "exp_1", "exp_2"),
    )
    placed = (
        P(REP_EXP, None),
        P(),
        P(None, EXP),
        P(None, EXP),
        P(EXP, None),
        P(REP_EXP, None),
        P(),
        P(REP_EXP, None),
        P(REP_EXP, None),
        P(EXP, None, None),
        P(EXP, None, None),
        P(EXP, None, None),
    )
    return jax.shard_map(
        shards,
        mesh=finer,
        in_specs=placed,
        out_specs=(P(REP_EXP, None), P(REP_EXP, None)),
        check_vma=False,
    )
```

```python
import jax
import jax.numpy as jnp
from jax import lax
from jax.experimental import pallas as pl
from jax.experimental.pallas import tpu as pltpu
from jax.sharding import Mesh
from jax.sharding import PartitionSpec as P


EXPERTS = 16
RING = 8
CORES = 2
EXP = ("exp_0", "exp_1", "exp_2")
REP_EXP = ("rep", "exp_0", "exp_1", "exp_2")


def pairs_along(stage, partner):
    pairs = []
    for x in range(RING):
        for y in range(RING):
            for c in range(CORES):
                along_x = (stage == 2) == (c == 0)
                to_x = partner(x) if along_x else x
                to_y = y if along_x else partner(y)
                pairs.append(((x * RING + y) * CORES + c, (to_x * RING + to_y) * CORES + c))
    return pairs


def even_partner(i):
    return i ^ 1


def odd_partner(i):
    return (((i + 1) % RING) ^ 1) - 1 if i else RING - 1


def over_even(array):
    return lax.ppermute(array, EXP, pairs_along(2, even_partner))


def over_odd(array):
    return lax.ppermute(array, EXP, pairs_along(2, odd_partner))


def swap_cores(array):
    devices = RING * RING * CORES
    return lax.ppermute(array, EXP, [(i, i ^ 1) for i in range(devices)])


def normed(values, gain_vec):
    return values * lax.rsqrt(jnp.mean(values * values, axis=-1, keepdims=True) + 1e-06) * gain_vec


GROUPS = ((0, 1, -1), (2, -2), (3, -3), (4,))


def stage_1_groups():
    first = [[(x * RING + y) * CORES for y in range(RING)] for x in range(RING)]
    second = [[(x * RING + y) * CORES + 1 for x in range(RING)] for y in range(RING)]
    return first + second


def exchange(blocks):
    return lax.all_to_all(
        blocks, EXP, split_axis=0, concat_axis=0, tiled=True, axis_index_groups=stage_1_groups()
    )


def gather_ring(block, cut):
    slots = {0: block}
    for k in (1, 2, 3):
        slots[k] = over_even(slots[1 - k])
        slots[-k] = over_odd(slots[k - 1])
    low = over_even(slots[-3][:, :cut])
    high = over_odd(slots[3][:, cut:])
    slots[4] = (low, high)
    return slots


def scatter_ring(own, other, streams):
    count = len(streams) - 1
    cuts = [(hi - lo) // 2 for lo, hi in zip(streams, streams[1:])]

    def part(k, i):
        at = slice(streams[i], streams[i + 1])
        return own[k][:, at].astype(jnp.float32) + other[k][:, at].astype(jnp.float32)

    low, high = [None] * count, [None] * count
    for i in range(count):
        far = part(4, i).astype(jnp.bfloat16)
        low[i] = over_even(far[:, : cuts[i]])
        high[i] = over_odd(far[:, cuts[i] :])
    for i in range(count):
        first, second = low[i].astype(jnp.float32), high[i].astype(jnp.float32)
        low[i] = jnp.concatenate([part(-3, i)[:, : cuts[i]] + first, part(-3, i)[:, cuts[i] :]], 1)
        high[i] = jnp.concatenate([part(3, i)[:, : cuts[i]], part(3, i)[:, cuts[i] :] + second], 1)
    for k in (2, 1, 0):
        for i in range(count):
            one, two = low[i].astype(jnp.bfloat16), high[i].astype(jnp.bfloat16)
            one = over_even(one) if k == 1 else over_odd(one)
            two = over_odd(two) if k == 1 else over_even(two)
            low[i], high[i] = one, two
        if k:
            side = 1 if k == 2 else -1
            for i in range(count):
                low[i] = part(side * k, i) + low[i].astype(jnp.float32)
                high[i] = part(-side * k, i) + high[i].astype(jnp.float32)
    return low, high


def layers(own, other, a_count, weights, pick, cut):
    units = pick.shape[1]
    width, dense_units = weights[2].shape[1], weights[2].shape[0]
    extra = dense_units - units
    full = width + units
    parts = []
    slots = 0
    for block in own + other:
        if isinstance(block, tuple):
            parts += [(block[0], slots, 0, cut), (block[1], slots, cut, None)]
        else:
            parts.append((block, slots, 0, None))
        slots += 1
    rows = parts[0][0].shape[0]
    b_count = rows - a_count
    half = slots // 2
    n_blocks = len(parts)
    inputs = [p[0] for p in parts] + list(weights) + [pick]
    n_in = len(inputs)
    chunk = 1792

    def body(*refs):
        ins = refs[:n_in]
        own_ref, other_ref = refs[n_in : n_in + 2]
        gate, up, da, e_gate, e_up, db = ins[n_blocks : n_blocks + 6]
        xa, xb, a_acc, b_acc, ha, hb, sems = refs[n_in + 2 :]
        a_copies, b_copies = [], []
        for i, (_, slot, lo, hi) in enumerate(parts):
            a_cols = pl.ds(lo, (width if hi is None else hi) - lo)
            b_cols = pl.ds(lo, (full if hi is None else hi) - lo)
            from_a = ins[i].at[pl.ds(0, a_count), pl.ds(0, a_cols.size)]
            from_b = ins[i].at[pl.ds(a_count, b_count), :]
            a_copies.append(
                pltpu.make_async_copy(from_a, xa.at[pl.ds(slot * a_count, a_count), a_cols], sems.at[2 * i])
            )
            b_copies.append(
                pltpu.make_async_copy(from_b, xb.at[pl.ds(slot * b_count, b_count), b_cols], sems.at[2 * i + 1])
            )
        for c in b_copies + a_copies:
            c.start()
        a_acc[...] = jnp.zeros_like(a_acc)
        b_acc[...] = jnp.zeros_like(b_acc)
        for c in b_copies:
            c.wait()

        def b_step(i, carry):
            at = pl.ds(pl.multiple_of(i * chunk, chunk), chunk)
            w = jnp.concatenate([e_gate[at, :], e_up[at, :]], 1)
            b_acc[...] += jnp.dot(xb[:, at], w, preferred_element_type=jnp.float32)
            return carry

        lax.fori_loop(0, width // chunk, b_step, 0)
        g = b_acc[:, :units]
        value = g * (1.0 / (1.0 + jnp.exp(-g))) * b_acc[:, units:]
        tail = xb[:, width:].astype(jnp.float32) * ins[n_in - 1][...]
        hb[...] = (value * jnp.sum(tail, axis=1, keepdims=True)).astype(jnp.bfloat16)
        for c in a_copies:
            c.wait()

        def a_step(i, carry):
            at = pl.ds(pl.multiple_of(i * chunk, chunk), chunk)
            w = jnp.concatenate([gate[:units, at], up[:units, at], gate[units:, at], up[units:, at]], 0)
            a_acc[...] += lax.dot_general(
                xa[:, at], w, (((1,), (1,)), ((), ())), preferred_element_type=jnp.float32
            )
            return carry

        lax.fori_loop(0, width // chunk, a_step, 0)
        for lo, n, to in ((0, units, 0), (2 * units, extra, units)):
            g = a_acc[:, lo : lo + n]
            u = a_acc[:, lo + n : lo + 2 * n]
            ha[:, to : to + n] = (g * (1.0 / (1.0 + jnp.exp(-g))) * u).astype(jnp.bfloat16)

        def out_step(i, carry):
            at = pl.ds(pl.multiple_of(i * chunk, chunk), chunk)
            for lo, count, h, w in ((0, a_count, ha, da), (a_count, b_count, hb, db)):
                r = jnp.dot(h[...], w[:, at], preferred_element_type=jnp.float32).astype(jnp.bfloat16)
                for slot in range(slots):
                    ref = own_ref if slot < half else other_ref
                    to = pl.ds(slot % half * rows + lo, count)
                    ref[to, at] = r[slot * count : (slot + 1) * count]
            return carry

        lax.fori_loop(0, width // chunk, out_step, 0)

    hbm_spec = pl.BlockSpec(memory_space=pltpu.HBM)
    vmem_spec = pl.BlockSpec(memory_space=pltpu.VMEM)
    a_total, b_total = slots * a_count, slots * b_count
    scratch = [
        ((a_total, width), jnp.bfloat16),
        ((b_total, full), jnp.bfloat16),
        ((a_total, 2 * dense_units), jnp.float32),
        ((b_total, 2 * units), jnp.float32),
        ((a_total, dense_units), jnp.bfloat16),
        ((b_total, units), jnp.bfloat16),
    ]
    return pl.pallas_call(
        body,
        in_specs=[hbm_spec] * n_blocks + [vmem_spec] * 7,
        out_specs=[vmem_spec] * 2,
        out_shape=[jax.ShapeDtypeStruct((half * rows, width), jnp.bfloat16)] * 2,
        scratch_shapes=[pltpu.VMEM(*s) for s in scratch]
        + [pltpu.SemaphoreType.DMA((2 * n_blocks,))],
        cost_estimate=pl.CostEstimate(
            flops=6 * width * (a_total * dense_units + b_total * units),
            bytes_accessed=6 * (dense_units + units) * width + 4 * (a_total + b_total) * width,
            transcendentals=0,
        ),
        compiler_params=pltpu.CompilerParams(vmem_limit_bytes=14 * 1024 * 1024),
    )(*inputs)


def prepare(a_tokens, a_gain, b_tokens, b_gain, expert_ids, route_weights):
    a_rows, width = a_tokens.shape
    rows = a_rows + b_tokens.shape[0]
    lanes = 128
    full = width + lanes
    inputs = (a_tokens, a_gain[None], b_tokens, b_gain[None], expert_ids, route_weights)

    def body(*refs):
        out_ref, hold, value = refs[6:9]
        held, sems = refs[9:15], refs[15]
        copies = [pltpu.make_async_copy(refs[i], held[i], sems.at[i]) for i in range(6)]
        for c in copies:
            c.start()
        for c in copies:
            c.wait()
        a_ref, ag_ref, b_ref, bg_ref, id_ref, w_ref = held
        hold[:a_rows, :width] = normed(a_ref[...].astype(jnp.float32), ag_ref[...])
        hold[:a_rows, width:] = jnp.zeros((a_rows, lanes), jnp.float32)
        hold[a_rows:rows, :width] = normed(b_ref[...].astype(jnp.float32), bg_ref[...])
        lane = lax.broadcasted_iota(jnp.int32, (rows - a_rows, lanes), 1)
        expert = lane & (EXPERTS - 1)
        weight = jnp.zeros((rows - a_rows, lanes), jnp.float32)
        for k in range(expert_ids.shape[1]):
            weight += jnp.where(id_ref[:, k : k + 1] == expert, w_ref[:, k : k + 1], 0.0)
        first = weight.astype(jnp.bfloat16).astype(jnp.float32)
        second = (weight - first).astype(jnp.bfloat16).astype(jnp.float32)
        third = weight - first - second
        part = jnp.where(lane < EXPERTS, first, jnp.where(lane < 2 * EXPERTS, second, third))
        hold[a_rows:rows, width:] = jnp.where(lane < 3 * EXPERTS, part, 0.0)
        value[...] = hold[:rows, :].astype(jnp.bfloat16)
        copies = [pltpu.make_async_copy(value, out_ref.at[i], sems.at[6 + i]) for i in range(RING)]
        for c in copies:
            c.start()
        for c in copies:
            c.wait()

    return pl.pallas_call(
        body,
        in_specs=[pl.BlockSpec(memory_space=pl.ANY)] * 6,
        out_specs=pl.BlockSpec(memory_space=pl.ANY),
        out_shape=jax.ShapeDtypeStruct((RING, rows, full), jnp.bfloat16),
        scratch_shapes=[pltpu.VMEM((8, full), jnp.float32), pltpu.VMEM((rows, full), jnp.bfloat16)]
        + [pltpu.VMEM(x.shape, x.dtype) for x in inputs]
        + [pltpu.SemaphoreType.DMA((6 + RING,))],
        compiler_params=pltpu.CompilerParams(vmem_limit_bytes=60 * 1024 * 1024),
        name="prepare",
    )(*inputs)


def pack(near, a_rows):
    places, rows, full = near.shape
    b_rows = rows - a_rows

    def body(near_ref, out_ref, hold):
        for i in range(places):
            value = near_ref[i].astype(jnp.float32)
            hold[pl.ds(i * a_rows, a_rows), :] = value[:a_rows]
            hold[pl.ds(places * a_rows + i * b_rows, b_rows), :] = value[a_rows:]
        out_ref[...] = hold[...].astype(jnp.bfloat16)

    vmem_spec = pl.BlockSpec(memory_space=pltpu.VMEM)
    return pl.pallas_call(
        body,
        in_specs=[vmem_spec],
        out_specs=vmem_spec,
        out_shape=jax.ShapeDtypeStruct((places * rows, full), jnp.bfloat16),
        scratch_shapes=[pltpu.VMEM((places * rows, full), jnp.float32)],
        compiler_params=pltpu.CompilerParams(vmem_limit_bytes=6 * 1024 * 1024),
        name="pack",
    )(near)


def touch(weights, pick):
    def body(*refs):
        refs[-1][...] = refs[-2][...]

    vmem_spec = pl.BlockSpec(memory_space=pltpu.VMEM)
    return pl.pallas_call(
        body,
        in_specs=[vmem_spec] * 7,
        out_specs=vmem_spec,
        out_shape=jax.ShapeDtypeStruct(pick.shape, pick.dtype),
        compiler_params=pltpu.CompilerParams(vmem_limit_bytes=1024 * 1024),
        name="touch",
    )(*weights, pick)


def unpack(own, other, low, high, streams, a_rows):
    total, width = own.shape
    rows = total // RING
    b_rows = rows - a_rows
    count = len(streams) - 1

    def body(*refs):
        own_ref, other_ref = refs[:2]
        lows, highs = refs[2 : 2 + count], refs[2 + count : 2 + 2 * count]
        out_ref, hold, one = refs[2 + 2 * count :]
        for i in range(count):
            at = slice(streams[i], streams[i + 1])
            hold[:, at] = (
                own_ref[:, at].astype(jnp.float32)
                + other_ref[:, at].astype(jnp.float32)
                + lows[i][...].astype(jnp.float32)
                + highs[i][...].astype(jnp.float32)
            )
        for j in range(RING):
            one[:a_rows] = hold[pl.ds(j * a_rows, a_rows), :]
            one[a_rows:rows] = hold[pl.ds(RING * a_rows + j * b_rows, b_rows), :]
            out_ref[j] = one[:rows].astype(jnp.bfloat16)

    vmem_spec = pl.BlockSpec(memory_space=pltpu.VMEM)
    return pl.pallas_call(
        body,
        in_specs=[vmem_spec] * (2 + 2 * count),
        out_specs=vmem_spec,
        out_shape=jax.ShapeDtypeStruct((RING, rows, width), jnp.bfloat16),
        scratch_shapes=[pltpu.VMEM((total, width), jnp.float32), pltpu.VMEM((8, width), jnp.float32)],
        compiler_params=pltpu.CompilerParams(vmem_limit_bytes=6 * 1024 * 1024),
        name="unpack",
    )(own, other, *low, *high)


def finish(pieces, a_tokens, b_tokens):
    a_rows, width = a_tokens.shape
    rows = pieces.shape[1]

    def body(piece_ref, a_ref, b_ref, a_out, b_out, hold):
        value = piece_ref[0].astype(jnp.float32)
        for j in range(1, RING):
            value = value + piece_ref[j].astype(jnp.float32)
        hold[:rows] = value
        a_out[...] = (a_ref[...].astype(jnp.float32) + hold[:a_rows]).astype(jnp.bfloat16)
        b_out[...] = (b_ref[...].astype(jnp.float32) + hold[a_rows:rows]).astype(jnp.bfloat16)

    vmem_spec = pl.BlockSpec(memory_space=pltpu.VMEM)
    return pl.pallas_call(
        body,
        in_specs=[vmem_spec] * 3,
        out_specs=[vmem_spec] * 2,
        out_shape=[
            jax.ShapeDtypeStruct(a_tokens.shape, jnp.bfloat16),
            jax.ShapeDtypeStruct(b_tokens.shape, jnp.bfloat16),
        ],
        scratch_shapes=[pltpu.VMEM((8, width), jnp.float32)],
        compiler_params=pltpu.CompilerParams(vmem_limit_bytes=2 * 1024 * 1024),
        name="finish",
    )(pieces, a_tokens, b_tokens)


def shards(
    a_tokens,
    a_gain,
    dense_gate,
    dense_up,
    dense_down,
    b_tokens,
    b_gain,
    expert_ids,
    route_weights,
    expert_gate,
    expert_up,
    expert_down,
):
    devices = lax.axis_size(EXP)
    group_size = devices // EXPERTS
    width = b_tokens.shape[1]
    a_rows = a_tokens.shape[0]
    ready = prepare(a_tokens, a_gain, b_tokens, b_gain, expert_ids, route_weights)
    full = ready.shape[2]
    block = pack(exchange(ready), a_rows)
    cut = width // 2
    slots = gather_ring(block, cut)
    swapped = {
        k: tuple(swap_cores(p) for p in s) if isinstance(s, tuple) else swap_cores(s)
        for k, s in slots.items()
    }
    expert = lax.axis_index(EXP) // group_size
    lanes = jnp.arange(full - width)
    pick = ((lanes % EXPERTS == expert) & (lanes < 3 * EXPERTS)).astype(jnp.float32)[None, :]
    weights = (
        dense_gate.T,
        dense_up.T,
        dense_down,
        expert_gate[0],
        expert_up[0],
        expert_down[0],
    )
    pick = touch(weights, pick)
    own, other = {}, {}
    rows = block.shape[0]
    for group in GROUPS:
        mine, theirs = layers(
            [slots[k] for k in group],
            [swapped[k] for k in group],
            RING * a_rows,
            weights,
            pick,
            cut,
        )
        theirs = swap_cores(theirs)
        for i, k in enumerate(group):
            own[k] = mine[i * rows : (i + 1) * rows]
            other[k] = theirs[i * rows : (i + 1) * rows]
    streams = (0, width * 4 // 7, width)
    low, high = scatter_ring(own, other, streams)
    pieces = unpack(own[0], other[0], low, high, streams, a_rows)
    return tuple(finish(exchange(pieces), a_tokens, b_tokens))


def solution(mesh):
    finer = Mesh(
        mesh.devices.reshape(mesh.shape["rep"], RING, RING, CORES),
        ("rep", "exp_0", "exp_1", "exp_2"),
    )
    placed = (
        P(REP_EXP, None),
        P(),
        P(None, EXP),
        P(None, EXP),
        P(EXP, None),
        P(REP_EXP, None),
        P(),
        P(REP_EXP, None),
        P(REP_EXP, None),
        P(EXP, None, None),
        P(EXP, None, None),
        P(EXP, None, None),
    )
    return jax.shard_map(
        shards,
        mesh=finer,
        in_specs=placed,
        out_specs=(P(REP_EXP, None), P(REP_EXP, None)),
        check_vma=False,
    )
```

```python
import jax
import jax.numpy as jnp
from jax import lax
from jax.experimental import pallas as pl
from jax.experimental.pallas import tpu as pltpu
from jax.sharding import Mesh
from jax.sharding import PartitionSpec as P


EXPERTS = 16
RING = 8
CORES = 2
EXP = ("exp_0", "exp_1", "exp_2")
REP_EXP = ("rep", "exp_0", "exp_1", "exp_2")


def pairs_along(stage, partner):
    pairs = []
    for x in range(RING):
        for y in range(RING):
            for c in range(CORES):
                along_x = (stage == 2) == (c == 0)
                to_x = partner(x) if along_x else x
                to_y = y if along_x else partner(y)
                pairs.append(((x * RING + y) * CORES + c, (to_x * RING + to_y) * CORES + c))
    return pairs


def even_partner(i):
    return i ^ 1


def odd_partner(i):
    return (((i + 1) % RING) ^ 1) - 1 if i else RING - 1


def over_even(array):
    return lax.ppermute(array, EXP, pairs_along(2, even_partner))


def over_odd(array):
    return lax.ppermute(array, EXP, pairs_along(2, odd_partner))


def swap_cores(array):
    devices = RING * RING * CORES
    return lax.ppermute(array, EXP, [(i, i ^ 1) for i in range(devices)])


def normed(values, gain_vec):
    return values * lax.rsqrt(jnp.mean(values * values, axis=-1, keepdims=True) + 1e-06) * gain_vec


GROUPS = ((0, 1, -1), (2, -2), (3, -3), (4,))


def stage_1_groups():
    first = [[(x * RING + y) * CORES for y in range(RING)] for x in range(RING)]
    second = [[(x * RING + y) * CORES + 1 for x in range(RING)] for y in range(RING)]
    return first + second


def exchange(blocks):
    return lax.all_to_all(
        blocks, EXP, split_axis=0, concat_axis=0, tiled=True, axis_index_groups=stage_1_groups()
    )


def gather_ring(block, cut):
    slots = {0: block}
    for k in (1, 2, 3):
        slots[k] = over_even(slots[1 - k])
        slots[-k] = over_odd(slots[k - 1])
    low = over_even(slots[-3][:, :cut])
    high = over_odd(slots[3][:, cut:])
    slots[4] = (low, high)
    return slots


def scatter_ring(own, other, streams):
    count = len(streams) - 1
    cuts = [(hi - lo) // 2 for lo, hi in zip(streams, streams[1:])]

    def part(k, i):
        at = slice(streams[i], streams[i + 1])
        return own[k][:, at].astype(jnp.float32) + other[k][:, at].astype(jnp.float32)

    low, high = [None] * count, [None] * count
    for i in range(count):
        far = part(4, i).astype(jnp.bfloat16)
        low[i] = over_even(far[:, : cuts[i]])
        high[i] = over_odd(far[:, cuts[i] :])
    for i in range(count):
        first, second = low[i].astype(jnp.float32), high[i].astype(jnp.float32)
        low[i] = jnp.concatenate([part(-3, i)[:, : cuts[i]] + first, part(-3, i)[:, cuts[i] :]], 1)
        high[i] = jnp.concatenate([part(3, i)[:, : cuts[i]], part(3, i)[:, cuts[i] :] + second], 1)
    for k in (2, 1, 0):
        for i in range(count):
            one, two = low[i].astype(jnp.bfloat16), high[i].astype(jnp.bfloat16)
            one = over_even(one) if k == 1 else over_odd(one)
            two = over_odd(two) if k == 1 else over_even(two)
            low[i], high[i] = one, two
        if k:
            side = 1 if k == 2 else -1
            for i in range(count):
                low[i] = part(side * k, i) + low[i].astype(jnp.float32)
                high[i] = part(-side * k, i) + high[i].astype(jnp.float32)
    return low, high


def layers(own, other, a_count, weights, pick, cut):
    units = pick.shape[1]
    width, dense_units = weights[2].shape[1], weights[2].shape[0]
    extra = dense_units - units
    full = width + units
    parts = []
    slots = 0
    for block in own + other:
        if isinstance(block, tuple):
            parts += [(block[0], slots, 0, cut), (block[1], slots, cut, None)]
        else:
            parts.append((block, slots, 0, None))
        slots += 1
    rows = parts[0][0].shape[0]
    b_count = rows - a_count
    half = slots // 2
    n_blocks = len(parts)
    inputs = [p[0] for p in parts] + list(weights) + [pick]
    n_in = len(inputs)
    chunk = 1792

    def body(*refs):
        ins = refs[:n_in]
        own_ref, other_ref = refs[n_in : n_in + 2]
        gate, up, da, e_gate, e_up, db = ins[n_blocks : n_blocks + 6]
        xa, xb, a_acc, b_acc, ha, hb, sems = refs[n_in + 2 :]
        a_copies, b_copies = [], []
        for i, (_, slot, lo, hi) in enumerate(parts):
            a_cols = pl.ds(lo, (width if hi is None else hi) - lo)
            b_cols = pl.ds(lo, (full if hi is None else hi) - lo)
            from_a = ins[i].at[pl.ds(0, a_count), pl.ds(0, a_cols.size)]
            from_b = ins[i].at[pl.ds(a_count, b_count), :]
            a_copies.append(
                pltpu.make_async_copy(from_a, xa.at[pl.ds(slot * a_count, a_count), a_cols], sems.at[2 * i])
            )
            b_copies.append(
                pltpu.make_async_copy(from_b, xb.at[pl.ds(slot * b_count, b_count), b_cols], sems.at[2 * i + 1])
            )
        for c in b_copies + a_copies:
            c.start()
        a_acc[...] = jnp.zeros_like(a_acc)
        b_acc[...] = jnp.zeros_like(b_acc)
        for c in b_copies:
            c.wait()

        def b_step(i, carry):
            at = pl.ds(pl.multiple_of(i * chunk, chunk), chunk)
            w = jnp.concatenate([e_gate[at, :], e_up[at, :]], 1)
            b_acc[...] += jnp.dot(xb[:, at], w, preferred_element_type=jnp.float32)
            return carry

        lax.fori_loop(0, width // chunk, b_step, 0)
        g = b_acc[:, :units]
        value = g * (1.0 / (1.0 + jnp.exp(-g))) * b_acc[:, units:]
        tail = xb[:, width:].astype(jnp.float32) * ins[n_in - 1][...]
        hb[...] = (value * jnp.sum(tail, axis=1, keepdims=True)).astype(jnp.bfloat16)
        for c in a_copies:
            c.wait()

        def a_step(i, carry):
            at = pl.ds(pl.multiple_of(i * chunk, chunk), chunk)
            w = jnp.concatenate([gate[:units, at], up[:units, at], gate[units:, at], up[units:, at]], 0)
            a_acc[...] += lax.dot_general(
                xa[:, at], w, (((1,), (1,)), ((), ())), preferred_element_type=jnp.float32
            )
            return carry

        lax.fori_loop(0, width // chunk, a_step, 0)
        for lo, n, to in ((0, units, 0), (2 * units, extra, units)):
            g = a_acc[:, lo : lo + n]
            u = a_acc[:, lo + n : lo + 2 * n]
            ha[:, to : to + n] = (g * (1.0 / (1.0 + jnp.exp(-g))) * u).astype(jnp.bfloat16)

        def out_step(i, carry):
            at = pl.ds(pl.multiple_of(i * chunk, chunk), chunk)
            for lo, count, h, w in ((0, a_count, ha, da), (a_count, b_count, hb, db)):
                r = jnp.dot(h[...], w[:, at], preferred_element_type=jnp.float32).astype(jnp.bfloat16)
                for slot in range(slots):
                    ref = own_ref if slot < half else other_ref
                    to = pl.ds(slot % half * rows + lo, count)
                    ref[to, at] = r[slot * count : (slot + 1) * count]
            return carry

        lax.fori_loop(0, width // chunk, out_step, 0)

    hbm_spec = pl.BlockSpec(memory_space=pltpu.HBM)
    vmem_spec = pl.BlockSpec(memory_space=pltpu.VMEM)
    a_total, b_total = slots * a_count, slots * b_count
    scratch = [
        ((a_total, width), jnp.bfloat16),
        ((b_total, full), jnp.bfloat16),
        ((a_total, 2 * dense_units), jnp.float32),
        ((b_total, 2 * units), jnp.float32),
        ((a_total, dense_units), jnp.bfloat16),
        ((b_total, units), jnp.bfloat16),
    ]
    return pl.pallas_call(
        body,
        in_specs=[hbm_spec] * n_blocks + [vmem_spec] * 7,
        out_specs=[vmem_spec] * 2,
        out_shape=[jax.ShapeDtypeStruct((half * rows, width), jnp.bfloat16)] * 2,
        scratch_shapes=[pltpu.VMEM(*s) for s in scratch]
        + [pltpu.SemaphoreType.DMA((2 * n_blocks,))],
        cost_estimate=pl.CostEstimate(
            flops=6 * width * (a_total * dense_units + b_total * units),
            bytes_accessed=6 * (dense_units + units) * width + 4 * (a_total + b_total) * width,
            transcendentals=0,
        ),
        compiler_params=pltpu.CompilerParams(vmem_limit_bytes=14 * 1024 * 1024),
    )(*inputs)


def fine_size(a_rows, b_rows, a_width, b_width):
    return -(-(a_rows * a_width + b_rows * b_width) // (128 * 16)) * 16


def fine_parts(a_rows, b_rows, a_width, b_width):
    a_tiles = a_width // 128
    parts = [(t * a_rows, 0, a_rows, t) for t in range(a_tiles)]
    return parts + [
        (a_tiles * a_rows + t * b_rows, a_rows, b_rows, t) for t in range(b_width // 128)
    ]


def prepare(a_tokens, a_gain, b_tokens, b_gain, expert_ids, route_weights):
    a_rows, width = a_tokens.shape
    rows = a_rows + b_tokens.shape[0]
    lanes = 128
    full = width + lanes
    fine_rows = fine_size(a_rows, rows - a_rows, width, full)
    inputs = (a_tokens, a_gain[None], b_tokens, b_gain[None], expert_ids, route_weights)

    def body(*refs):
        out_ref, hold, fine, value = refs[6:10]
        held, sems = refs[10:16], refs[16]
        copies = [pltpu.make_async_copy(refs[i], held[i], sems.at[i]) for i in range(6)]
        for c in copies:
            c.start()
        for c in copies:
            c.wait()
        a_ref, ag_ref, b_ref, bg_ref, id_ref, w_ref = held
        hold[:a_rows, :width] = normed(a_ref[...].astype(jnp.float32), ag_ref[...])
        hold[a_rows:rows, :width] = normed(b_ref[...].astype(jnp.float32), bg_ref[...])
        lane = lax.broadcasted_iota(jnp.int32, (rows - a_rows, lanes), 1)
        expert = lane & (EXPERTS - 1)
        weight = jnp.zeros((rows - a_rows, lanes), jnp.float32)
        for k in range(expert_ids.shape[1]):
            weight += jnp.where(id_ref[:, k : k + 1] == expert, w_ref[:, k : k + 1], 0.0)
        first = weight.astype(jnp.bfloat16).astype(jnp.float32)
        second = (weight - first).astype(jnp.bfloat16).astype(jnp.float32)
        third = weight - first - second
        part = jnp.where(lane < EXPERTS, first, jnp.where(lane < 2 * EXPERTS, second, third))
        hold[a_rows:rows, width:] = jnp.where(lane < 3 * EXPERTS, part, 0.0)
        fine[pl.ds(fine_rows - 16, 16), :] = jnp.zeros((16, lanes), jnp.float32)
        for to, lo, n, t in fine_parts(a_rows, rows - a_rows, width, full):
            fine[pl.ds(to, n), :] = hold[pl.ds(lo, n), pl.ds(t * lanes, lanes)]
        value[...] = fine[...].astype(jnp.bfloat16)
        copies = [pltpu.make_async_copy(value, out_ref.at[i], sems.at[6 + i]) for i in range(RING)]
        for c in copies:
            c.start()
        for c in copies:
            c.wait()

    return pl.pallas_call(
        body,
        in_specs=[pl.BlockSpec(memory_space=pl.ANY)] * 6,
        out_specs=pl.BlockSpec(memory_space=pl.ANY),
        out_shape=jax.ShapeDtypeStruct((RING, fine_rows, lanes), jnp.bfloat16),
        scratch_shapes=[pltpu.VMEM((8, full), jnp.float32), pltpu.VMEM((fine_rows, lanes), jnp.float32)]
        + [pltpu.VMEM((fine_rows, lanes), jnp.bfloat16)]
        + [pltpu.VMEM(x.shape, x.dtype) for x in inputs]
        + [pltpu.SemaphoreType.DMA((6 + RING,))],
        compiler_params=pltpu.CompilerParams(vmem_limit_bytes=60 * 1024 * 1024),
        name="prepare",
    )(*inputs)


def pack(near, a_rows, b_rows, width):
    places, fine_rows, lanes = near.shape
    full = width + lanes
    rows = a_rows + b_rows

    def body(near_ref, out_ref, fine, hold):
        hold[pl.ds(0, places * a_rows), pl.ds(width, lanes)] = jnp.zeros(
            (places * a_rows, lanes), jnp.float32
        )
        for i in range(places):
            fine[...] = near_ref[i].astype(jnp.float32)
            for at, lo, n, t in fine_parts(a_rows, b_rows, width, full):
                to = i * a_rows if lo == 0 else places * a_rows + i * b_rows
                hold[pl.ds(to, n), pl.ds(t * lanes, lanes)] = fine[pl.ds(at, n), :]
        out_ref[...] = hold[...].astype(jnp.bfloat16)

    vmem_spec = pl.BlockSpec(memory_space=pltpu.VMEM)
    return pl.pallas_call(
        body,
        in_specs=[vmem_spec],
        out_specs=vmem_spec,
        out_shape=jax.ShapeDtypeStruct((places * rows, full), jnp.bfloat16),
        scratch_shapes=[
            pltpu.VMEM((fine_rows, lanes), jnp.float32),
            pltpu.VMEM((places * rows, full), jnp.float32),
        ],
        compiler_params=pltpu.CompilerParams(vmem_limit_bytes=6 * 1024 * 1024),
        name="pack",
    )(near)


def touch(weights, pick):
    def body(*refs):
        refs[-1][...] = refs[-2][...]

    vmem_spec = pl.BlockSpec(memory_space=pltpu.VMEM)
    return pl.pallas_call(
        body,
        in_specs=[vmem_spec] * 7,
        out_specs=vmem_spec,
        out_shape=jax.ShapeDtypeStruct(pick.shape, pick.dtype),
        compiler_params=pltpu.CompilerParams(vmem_limit_bytes=1024 * 1024),
        name="touch",
    )(*weights, pick)


def unpack(own, other, low, high, streams, a_rows):
    total, width = own.shape
    rows = total // RING
    b_rows = rows - a_rows
    count = len(streams) - 1
    lanes = 128
    fine_rows = fine_size(a_rows, b_rows, width, width)

    def body(*refs):
        own_ref, other_ref = refs[:2]
        lows, highs = refs[2 : 2 + count], refs[2 + count : 2 + 2 * count]
        out_ref, hold, one = refs[2 + 2 * count :]
        for i in range(count):
            at = slice(streams[i], streams[i + 1])
            hold[:, at] = (
                own_ref[:, at].astype(jnp.float32)
                + other_ref[:, at].astype(jnp.float32)
                + lows[i][...].astype(jnp.float32)
                + highs[i][...].astype(jnp.float32)
            )
        for j in range(RING):
            for to, lo, n, t in fine_parts(a_rows, b_rows, width, width):
                at = j * a_rows if lo == 0 else RING * a_rows + j * b_rows
                one[pl.ds(to, n), :] = hold[pl.ds(at, n), pl.ds(t * lanes, lanes)]
            out_ref[j] = one[...].astype(jnp.bfloat16)

    vmem_spec = pl.BlockSpec(memory_space=pltpu.VMEM)
    return pl.pallas_call(
        body,
        in_specs=[vmem_spec] * (2 + 2 * count),
        out_specs=vmem_spec,
        out_shape=jax.ShapeDtypeStruct((RING, fine_rows, lanes), jnp.bfloat16),
        scratch_shapes=[pltpu.VMEM((total, width), jnp.float32), pltpu.VMEM((fine_rows, lanes), jnp.float32)],
        compiler_params=pltpu.CompilerParams(vmem_limit_bytes=6 * 1024 * 1024),
        name="unpack",
    )(own, other, *low, *high)


def finish(pieces, a_tokens, b_tokens):
    a_rows, width = a_tokens.shape
    b_rows = b_tokens.shape[0]
    rows = a_rows + b_rows
    fine_rows, lanes = pieces.shape[1:]

    def body(piece_ref, a_ref, b_ref, a_out, b_out, fine, hold):
        value = piece_ref[0].astype(jnp.float32)
        for j in range(1, RING):
            value = value + piece_ref[j].astype(jnp.float32)
        fine[...] = value
        for at, lo, n, t in fine_parts(a_rows, b_rows, width, width):
            hold[pl.ds(lo, n), pl.ds(t * lanes, lanes)] = fine[pl.ds(at, n), :]
        a_out[...] = (a_ref[...].astype(jnp.float32) + hold[:a_rows]).astype(jnp.bfloat16)
        b_out[...] = (b_ref[...].astype(jnp.float32) + hold[a_rows:rows]).astype(jnp.bfloat16)

    vmem_spec = pl.BlockSpec(memory_space=pltpu.VMEM)
    return pl.pallas_call(
        body,
        in_specs=[vmem_spec] * 3,
        out_specs=[vmem_spec] * 2,
        out_shape=[
            jax.ShapeDtypeStruct(a_tokens.shape, jnp.bfloat16),
            jax.ShapeDtypeStruct(b_tokens.shape, jnp.bfloat16),
        ],
        scratch_shapes=[pltpu.VMEM((fine_rows, lanes), jnp.float32), pltpu.VMEM((8, width), jnp.float32)],
        compiler_params=pltpu.CompilerParams(vmem_limit_bytes=2 * 1024 * 1024),
        name="finish",
    )(pieces, a_tokens, b_tokens)


def shards(
    a_tokens,
    a_gain,
    dense_gate,
    dense_up,
    dense_down,
    b_tokens,
    b_gain,
    expert_ids,
    route_weights,
    expert_gate,
    expert_up,
    expert_down,
):
    devices = lax.axis_size(EXP)
    group_size = devices // EXPERTS
    width = b_tokens.shape[1]
    a_rows = a_tokens.shape[0]
    ready = prepare(a_tokens, a_gain, b_tokens, b_gain, expert_ids, route_weights)
    full = width + ready.shape[2]
    block = pack(exchange(ready), a_rows, b_tokens.shape[0], width)
    cut = width // 2
    slots = gather_ring(block, cut)
    swapped = {
        k: tuple(swap_cores(p) for p in s) if isinstance(s, tuple) else swap_cores(s)
        for k, s in slots.items()
    }
    expert = lax.axis_index(EXP) // group_size
    lanes = jnp.arange(full - width)
    pick = ((lanes % EXPERTS == expert) & (lanes < 3 * EXPERTS)).astype(jnp.float32)[None, :]
    weights = (
        dense_gate.T,
        dense_up.T,
        dense_down,
        expert_gate[0],
        expert_up[0],
        expert_down[0],
    )
    pick = touch(weights, pick)
    own, other = {}, {}
    rows = block.shape[0]
    for group in GROUPS:
        mine, theirs = layers(
            [slots[k] for k in group],
            [swapped[k] for k in group],
            RING * a_rows,
            weights,
            pick,
            cut,
        )
        theirs = swap_cores(theirs)
        for i, k in enumerate(group):
            own[k] = mine[i * rows : (i + 1) * rows]
            other[k] = theirs[i * rows : (i + 1) * rows]
    streams = (0, width * 4 // 7, width)
    low, high = scatter_ring(own, other, streams)
    pieces = unpack(own[0], other[0], low, high, streams, a_rows)
    return tuple(finish(exchange(pieces), a_tokens, b_tokens))


def solution(mesh):
    finer = Mesh(
        mesh.devices.reshape(mesh.shape["rep"], RING, RING, CORES),
        ("rep", "exp_0", "exp_1", "exp_2"),
    )
    placed = (
        P(REP_EXP, None),
        P(),
        P(None, EXP),
        P(None, EXP),
        P(EXP, None),
        P(REP_EXP, None),
        P(),
        P(REP_EXP, None),
        P(REP_EXP, None),
        P(EXP, None, None),
        P(EXP, None, None),
        P(EXP, None, None),
    )
    return jax.shard_map(
        shards,
        mesh=finer,
        in_specs=placed,
        out_specs=(P(REP_EXP, None), P(REP_EXP, None)),
        check_vma=False,
    )
```

```python
import jax
import jax.numpy as jnp
from jax import lax
from jax.experimental import pallas as pl
from jax.experimental.pallas import tpu as pltpu
from jax.sharding import Mesh
from jax.sharding import PartitionSpec as P


EXPERTS = 16
RING = 8
CORES = 2
EXP = ("exp_0", "exp_1", "exp_2")
REP_EXP = ("rep", "exp_0", "exp_1", "exp_2")


def pairs_along(stage, partner):
    pairs = []
    for x in range(RING):
        for y in range(RING):
            for c in range(CORES):
                along_x = (stage == 2) == (c == 0)
                to_x = partner(x) if along_x else x
                to_y = y if along_x else partner(y)
                pairs.append(((x * RING + y) * CORES + c, (to_x * RING + to_y) * CORES + c))
    return pairs


def even_partner(i):
    return i ^ 1


def odd_partner(i):
    return (((i + 1) % RING) ^ 1) - 1 if i else RING - 1


def over_even(array):
    return lax.ppermute(array, EXP, pairs_along(2, even_partner))


def over_odd(array):
    return lax.ppermute(array, EXP, pairs_along(2, odd_partner))


def swap_cores(array):
    devices = RING * RING * CORES
    return lax.ppermute(array, EXP, [(i, i ^ 1) for i in range(devices)])


def normed(values, gain_vec):
    return values * lax.rsqrt(jnp.mean(values * values, axis=-1, keepdims=True) + 1e-06) * gain_vec


GROUPS = ((0, 1, -1), (2, -2), (3, -3), (4,))


def stage_1_groups():
    first = [[(x * RING + y) * CORES for y in range(RING)] for x in range(RING)]
    second = [[(x * RING + y) * CORES + 1 for x in range(RING)] for y in range(RING)]
    return first + second


def exchange(blocks):
    return lax.all_to_all(
        blocks, EXP, split_axis=0, concat_axis=0, tiled=True, axis_index_groups=stage_1_groups()
    )


def gather_ring(block, cut):
    slots = {0: block}
    for k in (1, 2, 3):
        slots[k] = over_even(slots[1 - k])
        slots[-k] = over_odd(slots[k - 1])
    low = over_even(slots[-3][:, :cut])
    high = over_odd(slots[3][:, cut:])
    slots[4] = (low, high)
    return slots


def scatter_ring(own, other, cut):
    width = own[0].shape[1]
    head, tail = (0, cut), (cut, width)

    def part(k, cols):
        lo, hi = cols
        return own[k][:, lo:hi].astype(jnp.float32) + other[k][:, lo:hi].astype(jnp.float32)

    def add(k, cols, piece):
        return (part(k, cols) + piece.astype(jnp.float32)).astype(jnp.bfloat16)

    short_head = over_even(part(3, head).astype(jnp.bfloat16))
    short_tail = over_odd(part(-3, tail).astype(jnp.bfloat16))
    long_head = over_even(part(4, head).astype(jnp.bfloat16))
    long_tail = over_odd(part(4, tail).astype(jnp.bfloat16))
    for step, k in enumerate((2, 1, 0)):
        side = -1 if step == 0 else 1
        even, odd = (over_odd, over_even) if step == 0 else (over_even, over_odd)
        if k:
            short = add(side * k, head, short_head), add(-side * k, tail, short_tail)
            long_head, long_tail, *short = lax.optimization_barrier((long_head, long_tail, *short))
            short_head, short_tail = even(short[0]), odd(short[1])
        side = 1 if step == 1 else -1
        even, odd = (over_even, over_odd) if step == 1 else (over_odd, over_even)
        long_head = even(add(side * (k + 1), head, long_head))
        long_tail = odd(add(-side * (k + 1), tail, long_tail))
    return (long_head, short_tail), (short_head, long_tail)


def layers(own, other, a_count, weights, pick, cut):
    units = pick.shape[1]
    width, dense_units = weights[2].shape[1], weights[2].shape[0]
    extra = dense_units - units
    full = width + units
    parts = []
    slots = 0
    for block in own + other:
        if isinstance(block, tuple):
            parts += [(block[0], slots, 0, cut), (block[1], slots, cut, None)]
        else:
            parts.append((block, slots, 0, None))
        slots += 1
    rows = parts[0][0].shape[0]
    b_count = rows - a_count
    half = slots // 2
    n_blocks = len(parts)
    inputs = [p[0] for p in parts] + list(weights) + [pick]
    n_in = len(inputs)
    chunk = 1792

    def body(*refs):
        ins = refs[:n_in]
        own_ref, other_ref = refs[n_in : n_in + 2]
        gate, up, da, e_gate, e_up, db = ins[n_blocks : n_blocks + 6]
        xa, xb, a_acc, b_acc, ha, hb, sems = refs[n_in + 2 :]
        a_copies, b_copies = [], []
        for i, (_, slot, lo, hi) in enumerate(parts):
            a_cols = pl.ds(lo, (width if hi is None else hi) - lo)
            b_cols = pl.ds(lo, (full if hi is None else hi) - lo)
            from_a = ins[i].at[pl.ds(0, a_count), pl.ds(0, a_cols.size)]
            from_b = ins[i].at[pl.ds(a_count, b_count), :]
            a_copies.append(
                pltpu.make_async_copy(from_a, xa.at[pl.ds(slot * a_count, a_count), a_cols], sems.at[2 * i])
            )
            b_copies.append(
                pltpu.make_async_copy(from_b, xb.at[pl.ds(slot * b_count, b_count), b_cols], sems.at[2 * i + 1])
            )
        for c in b_copies + a_copies:
            c.start()
        a_acc[...] = jnp.zeros_like(a_acc)
        b_acc[...] = jnp.zeros_like(b_acc)
        for c in b_copies:
            c.wait()

        def b_step(i, carry):
            at = pl.ds(pl.multiple_of(i * chunk, chunk), chunk)
            w = jnp.concatenate([e_gate[at, :], e_up[at, :]], 1)
            b_acc[...] += jnp.dot(xb[:, at], w, preferred_element_type=jnp.float32)
            return carry

        lax.fori_loop(0, width // chunk, b_step, 0)
        g = b_acc[:, :units]
        value = g * (1.0 / (1.0 + jnp.exp(-g))) * b_acc[:, units:]
        tail = xb[:, width:].astype(jnp.float32) * ins[n_in - 1][...]
        hb[...] = (value * jnp.sum(tail, axis=1, keepdims=True)).astype(jnp.bfloat16)
        for c in a_copies:
            c.wait()

        def a_step(i, carry):
            at = pl.ds(pl.multiple_of(i * chunk, chunk), chunk)
            w = jnp.concatenate([gate[:units, at], up[:units, at], gate[units:, at], up[units:, at]], 0)
            a_acc[...] += lax.dot_general(
                xa[:, at], w, (((1,), (1,)), ((), ())), preferred_element_type=jnp.float32
            )
            return carry

        lax.fori_loop(0, width // chunk, a_step, 0)
        for lo, n, to in ((0, units, 0), (2 * units, extra, units)):
            g = a_acc[:, lo : lo + n]
            u = a_acc[:, lo + n : lo + 2 * n]
            ha[:, to : to + n] = (g * (1.0 / (1.0 + jnp.exp(-g))) * u).astype(jnp.bfloat16)

        def out_step(i, carry):
            at = pl.ds(pl.multiple_of(i * chunk, chunk), chunk)
            for lo, count, h, w in ((0, a_count, ha, da), (a_count, b_count, hb, db)):
                r = jnp.dot(h[...], w[:, at], preferred_element_type=jnp.float32).astype(jnp.bfloat16)
                for slot in range(slots):
                    ref = own_ref if slot < half else other_ref
                    to = pl.ds(slot % half * rows + lo, count)
                    ref[to, at] = r[slot * count : (slot + 1) * count]
            return carry

        lax.fori_loop(0, width // chunk, out_step, 0)

    hbm_spec = pl.BlockSpec(memory_space=pltpu.HBM)
    vmem_spec = pl.BlockSpec(memory_space=pltpu.VMEM)
    a_total, b_total = slots * a_count, slots * b_count
    scratch = [
        ((a_total, width), jnp.bfloat16),
        ((b_total, full), jnp.bfloat16),
        ((a_total, 2 * dense_units), jnp.float32),
        ((b_total, 2 * units), jnp.float32),
        ((a_total, dense_units), jnp.bfloat16),
        ((b_total, units), jnp.bfloat16),
    ]
    return pl.pallas_call(
        body,
        in_specs=[hbm_spec] * n_blocks + [vmem_spec] * 7,
        out_specs=[vmem_spec] * 2,
        out_shape=[jax.ShapeDtypeStruct((half * rows, width), jnp.bfloat16)] * 2,
        scratch_shapes=[pltpu.VMEM(*s) for s in scratch]
        + [pltpu.SemaphoreType.DMA((2 * n_blocks,))],
        cost_estimate=pl.CostEstimate(
            flops=6 * width * (a_total * dense_units + b_total * units),
            bytes_accessed=6 * (dense_units + units) * width + 4 * (a_total + b_total) * width,
            transcendentals=0,
        ),
        compiler_params=pltpu.CompilerParams(vmem_limit_bytes=14 * 1024 * 1024),
    )(*inputs)


def fine_size(a_rows, b_rows, a_width, b_width):
    return -(-(a_rows * a_width + b_rows * b_width) // (128 * 16)) * 16


def fine_parts(a_rows, b_rows, a_width, b_width):
    a_tiles = a_width // 128
    parts = [(t * a_rows, 0, a_rows, t) for t in range(a_tiles)]
    return parts + [
        (a_tiles * a_rows + t * b_rows, a_rows, b_rows, t) for t in range(b_width // 128)
    ]


def prepare(a_tokens, a_gain, b_tokens, b_gain, expert_ids, route_weights):
    a_rows, width = a_tokens.shape
    rows = a_rows + b_tokens.shape[0]
    lanes = 128
    full = width + lanes
    fine_rows = fine_size(a_rows, rows - a_rows, width, full)
    inputs = (a_tokens, a_gain[None], b_tokens, b_gain[None], expert_ids, route_weights)

    def body(*refs):
        out_ref, hold, fine, value = refs[6:10]
        held, sems = refs[10:16], refs[16]
        copies = [pltpu.make_async_copy(refs[i], held[i], sems.at[i]) for i in range(6)]
        for c in copies:
            c.start()
        for c in copies:
            c.wait()
        a_ref, ag_ref, b_ref, bg_ref, id_ref, w_ref = held
        hold[:a_rows, :width] = normed(a_ref[...].astype(jnp.float32), ag_ref[...])
        hold[a_rows:rows, :width] = normed(b_ref[...].astype(jnp.float32), bg_ref[...])
        lane = lax.broadcasted_iota(jnp.int32, (rows - a_rows, lanes), 1)
        expert = lane & (EXPERTS - 1)
        weight = jnp.zeros((rows - a_rows, lanes), jnp.float32)
        for k in range(expert_ids.shape[1]):
            weight += jnp.where(id_ref[:, k : k + 1] == expert, w_ref[:, k : k + 1], 0.0)
        first = weight.astype(jnp.bfloat16).astype(jnp.float32)
        second = (weight - first).astype(jnp.bfloat16).astype(jnp.float32)
        third = weight - first - second
        part = jnp.where(lane < EXPERTS, first, jnp.where(lane < 2 * EXPERTS, second, third))
        hold[a_rows:rows, width:] = jnp.where(lane < 3 * EXPERTS, part, 0.0)
        fine[pl.ds(fine_rows - 16, 16), :] = jnp.zeros((16, lanes), jnp.float32)
        for to, lo, n, t in fine_parts(a_rows, rows - a_rows, width, full):
            fine[pl.ds(to, n), :] = hold[pl.ds(lo, n), pl.ds(t * lanes, lanes)]
        value[...] = fine[...].astype(jnp.bfloat16)
        copies = [pltpu.make_async_copy(value, out_ref.at[i], sems.at[6 + i]) for i in range(RING)]
        for c in copies:
            c.start()
        for c in copies:
            c.wait()

    return pl.pallas_call(
        body,
        in_specs=[pl.BlockSpec(memory_space=pl.ANY)] * 6,
        out_specs=pl.BlockSpec(memory_space=pl.ANY),
        out_shape=jax.ShapeDtypeStruct((RING, fine_rows, lanes), jnp.bfloat16),
        scratch_shapes=[pltpu.VMEM((8, full), jnp.float32), pltpu.VMEM((fine_rows, lanes), jnp.float32)]
        + [pltpu.VMEM((fine_rows, lanes), jnp.bfloat16)]
        + [pltpu.VMEM(x.shape, x.dtype) for x in inputs]
        + [pltpu.SemaphoreType.DMA((6 + RING,))],
        compiler_params=pltpu.CompilerParams(vmem_limit_bytes=60 * 1024 * 1024),
        name="prepare",
    )(*inputs)


def pack(near, a_rows, b_rows, width):
    places, fine_rows, lanes = near.shape
    full = width + lanes
    rows = a_rows + b_rows

    def body(near_ref, out_ref, fine, hold):
        hold[pl.ds(0, places * a_rows), pl.ds(width, lanes)] = jnp.zeros(
            (places * a_rows, lanes), jnp.float32
        )
        for i in range(places):
            fine[...] = near_ref[i].astype(jnp.float32)
            for at, lo, n, t in fine_parts(a_rows, b_rows, width, full):
                to = i * a_rows if lo == 0 else places * a_rows + i * b_rows
                hold[pl.ds(to, n), pl.ds(t * lanes, lanes)] = fine[pl.ds(at, n), :]
        out_ref[...] = hold[...].astype(jnp.bfloat16)

    vmem_spec = pl.BlockSpec(memory_space=pltpu.VMEM)
    return pl.pallas_call(
        body,
        in_specs=[vmem_spec],
        out_specs=vmem_spec,
        out_shape=jax.ShapeDtypeStruct((places * rows, full), jnp.bfloat16),
        scratch_shapes=[
            pltpu.VMEM((fine_rows, lanes), jnp.float32),
            pltpu.VMEM((places * rows, full), jnp.float32),
        ],
        compiler_params=pltpu.CompilerParams(vmem_limit_bytes=6 * 1024 * 1024),
        name="pack",
    )(near)


def touch(weights, pick):
    def body(*refs):
        refs[-1][...] = refs[-2][...]

    vmem_spec = pl.BlockSpec(memory_space=pltpu.VMEM)
    return pl.pallas_call(
        body,
        in_specs=[vmem_spec] * 7,
        out_specs=vmem_spec,
        out_shape=jax.ShapeDtypeStruct(pick.shape, pick.dtype),
        compiler_params=pltpu.CompilerParams(vmem_limit_bytes=1024 * 1024),
        name="touch",
    )(*weights, pick)


def unpack(own, other, low, high, streams, a_rows):
    total, width = own.shape
    rows = total // RING
    b_rows = rows - a_rows
    count = len(streams) - 1
    lanes = 128
    fine_rows = fine_size(a_rows, b_rows, width, width)

    def body(*refs):
        own_ref, other_ref = refs[:2]
        lows, highs = refs[2 : 2 + count], refs[2 + count : 2 + 2 * count]
        out_ref, hold, one = refs[2 + 2 * count :]
        for i in range(count):
            at = slice(streams[i], streams[i + 1])
            hold[:, at] = (
                own_ref[:, at].astype(jnp.float32)
                + other_ref[:, at].astype(jnp.float32)
                + lows[i][...].astype(jnp.float32)
                + highs[i][...].astype(jnp.float32)
            )
        for j in range(RING):
            for to, lo, n, t in fine_parts(a_rows, b_rows, width, width):
                at = j * a_rows if lo == 0 else RING * a_rows + j * b_rows
                one[pl.ds(to, n), :] = hold[pl.ds(at, n), pl.ds(t * lanes, lanes)]
            out_ref[j] = one[...].astype(jnp.bfloat16)

    vmem_spec = pl.BlockSpec(memory_space=pltpu.VMEM)
    return pl.pallas_call(
        body,
        in_specs=[vmem_spec] * (2 + 2 * count),
        out_specs=vmem_spec,
        out_shape=jax.ShapeDtypeStruct((RING, fine_rows, lanes), jnp.bfloat16),
        scratch_shapes=[pltpu.VMEM((total, width), jnp.float32), pltpu.VMEM((fine_rows, lanes), jnp.float32)],
        compiler_params=pltpu.CompilerParams(vmem_limit_bytes=6 * 1024 * 1024),
        name="unpack",
    )(own, other, *low, *high)


def finish(pieces, a_tokens, b_tokens):
    a_rows, width = a_tokens.shape
    b_rows = b_tokens.shape[0]
    rows = a_rows + b_rows
    fine_rows, lanes = pieces.shape[1:]

    def body(piece_ref, a_ref, b_ref, a_out, b_out, fine, hold):
        value = piece_ref[0].astype(jnp.float32)
        for j in range(1, RING):
            value = value + piece_ref[j].astype(jnp.float32)
        fine[...] = value
        for at, lo, n, t in fine_parts(a_rows, b_rows, width, width):
            hold[pl.ds(lo, n), pl.ds(t * lanes, lanes)] = fine[pl.ds(at, n), :]
        a_out[...] = (a_ref[...].astype(jnp.float32) + hold[:a_rows]).astype(jnp.bfloat16)
        b_out[...] = (b_ref[...].astype(jnp.float32) + hold[a_rows:rows]).astype(jnp.bfloat16)

    vmem_spec = pl.BlockSpec(memory_space=pltpu.VMEM)
    return pl.pallas_call(
        body,
        in_specs=[vmem_spec] * 3,
        out_specs=[vmem_spec] * 2,
        out_shape=[
            jax.ShapeDtypeStruct(a_tokens.shape, jnp.bfloat16),
            jax.ShapeDtypeStruct(b_tokens.shape, jnp.bfloat16),
        ],
        scratch_shapes=[pltpu.VMEM((fine_rows, lanes), jnp.float32), pltpu.VMEM((8, width), jnp.float32)],
        compiler_params=pltpu.CompilerParams(vmem_limit_bytes=2 * 1024 * 1024),
        name="finish",
    )(pieces, a_tokens, b_tokens)


def shards(
    a_tokens,
    a_gain,
    dense_gate,
    dense_up,
    dense_down,
    b_tokens,
    b_gain,
    expert_ids,
    route_weights,
    expert_gate,
    expert_up,
    expert_down,
):
    devices = lax.axis_size(EXP)
    group_size = devices // EXPERTS
    width = b_tokens.shape[1]
    a_rows = a_tokens.shape[0]
    ready = prepare(a_tokens, a_gain, b_tokens, b_gain, expert_ids, route_weights)
    full = width + ready.shape[2]
    block = pack(exchange(ready), a_rows, b_tokens.shape[0], width)
    cut = width // 2
    slots = gather_ring(block, cut)
    swapped = {
        k: tuple(swap_cores(p) for p in s) if isinstance(s, tuple) else swap_cores(s)
        for k, s in slots.items()
    }
    expert = lax.axis_index(EXP) // group_size
    lanes = jnp.arange(full - width)
    pick = ((lanes % EXPERTS == expert) & (lanes < 3 * EXPERTS)).astype(jnp.float32)[None, :]
    weights = (
        dense_gate.T,
        dense_up.T,
        dense_down,
        expert_gate[0],
        expert_up[0],
        expert_down[0],
    )
    pick = touch(weights, pick)
    own, other = {}, {}
    rows = block.shape[0]
    for group in GROUPS:
        mine, theirs = layers(
            [slots[k] for k in group],
            [swapped[k] for k in group],
            RING * a_rows,
            weights,
            pick,
            cut,
        )
        theirs = swap_cores(theirs)
        for i, k in enumerate(group):
            own[k] = mine[i * rows : (i + 1) * rows]
            other[k] = theirs[i * rows : (i + 1) * rows]
    streams = (0, cut, width)
    low, high = scatter_ring(own, other, cut)
    pieces = unpack(own[0], other[0], low, high, streams, a_rows)
    return tuple(finish(exchange(pieces), a_tokens, b_tokens))


def solution(mesh):
    finer = Mesh(
        mesh.devices.reshape(mesh.shape["rep"], RING, RING, CORES),
        ("rep", "exp_0", "exp_1", "exp_2"),
    )
    placed = (
        P(REP_EXP, None),
        P(),
        P(None, EXP),
        P(None, EXP),
        P(EXP, None),
        P(REP_EXP, None),
        P(),
        P(REP_EXP, None),
        P(REP_EXP, None),
        P(EXP, None, None),
        P(EXP, None, None),
        P(EXP, None, None),
    )
    return jax.shard_map(
        shards,
        mesh=finer,
        in_specs=placed,
        out_specs=(P(REP_EXP, None), P(REP_EXP, None)),
        check_vma=False,
    )
```

```python
import jax
import jax.numpy as jnp
from jax import lax
from jax.experimental import pallas as pl
from jax.experimental.pallas import tpu as pltpu
from jax.sharding import Mesh
from jax.sharding import PartitionSpec as P


EXPERTS = 16
RING = 8
CORES = 2
EXP = ("exp_0", "exp_1", "exp_2")
REP_EXP = ("rep", "exp_0", "exp_1", "exp_2")


def pairs_along(stage, partner):
    pairs = []
    for x in range(RING):
        for y in range(RING):
            for c in range(CORES):
                along_x = (stage == 2) == (c == 0)
                to_x = partner(x) if along_x else x
                to_y = y if along_x else partner(y)
                pairs.append(((x * RING + y) * CORES + c, (to_x * RING + to_y) * CORES + c))
    return pairs


def even_partner(i):
    return i ^ 1


def odd_partner(i):
    return (((i + 1) % RING) ^ 1) - 1 if i else RING - 1


def over_even(array):
    return lax.ppermute(array, EXP, pairs_along(2, even_partner))


def over_odd(array):
    return lax.ppermute(array, EXP, pairs_along(2, odd_partner))


def swap_cores(array):
    devices = RING * RING * CORES
    return lax.ppermute(array, EXP, [(i, i ^ 1) for i in range(devices)])


def normed(values, gain_vec):
    return values * lax.rsqrt(jnp.mean(values * values, axis=-1, keepdims=True) + 1e-06) * gain_vec


GROUPS = ((0, 1, -1), (2, -2), (3, -3), (4,))


def stage_1_groups():
    first = [[(x * RING + y) * CORES for y in range(RING)] for x in range(RING)]
    second = [[(x * RING + y) * CORES + 1 for x in range(RING)] for y in range(RING)]
    return first + second


def exchange(blocks):
    return lax.all_to_all(
        blocks, EXP, split_axis=0, concat_axis=0, tiled=True, axis_index_groups=stage_1_groups()
    )


def gather_ring(block, cut):
    slots = {0: block}
    for k in (1, 2, 3):
        slots[k] = over_even(slots[1 - k])
        slots[-k] = over_odd(slots[k - 1])
    low = over_even(slots[-3][:, :cut])
    high = over_odd(slots[3][:, cut:])
    slots[4] = (low, high)
    return slots


def scatter_ring(own, other, cut):
    width = own[0].shape[1]
    head, tail = (0, cut), (cut, width)

    def part(k, cols):
        lo, hi = cols
        return own[k][:, lo:hi].astype(jnp.float32) + other[k][:, lo:hi].astype(jnp.float32)

    def add(k, cols, piece):
        return (part(k, cols) + piece.astype(jnp.float32)).astype(jnp.bfloat16)

    short_head = over_even(part(3, head).astype(jnp.bfloat16))
    short_tail = over_odd(part(-3, tail).astype(jnp.bfloat16))
    long_head = over_even(part(4, head).astype(jnp.bfloat16))
    long_tail = over_odd(part(4, tail).astype(jnp.bfloat16))
    for step, k in enumerate((2, 1, 0)):
        side = -1 if step == 0 else 1
        even, odd = (over_odd, over_even) if step == 0 else (over_even, over_odd)
        if k:
            short = add(side * k, head, short_head), add(-side * k, tail, short_tail)
            long_head, long_tail, *_ = lax.optimization_barrier((long_head, long_tail, *short))
            short_head = even(short[0])
            short_tail = odd(short[1])
        side = 1 if step == 1 else -1
        even, odd = (over_even, over_odd) if step == 1 else (over_odd, over_even)
        long = add(side * (k + 1), head, long_head), add(-side * (k + 1), tail, long_tail)
        long_head = even(long[0])
        long_tail = odd(long[1])
    return (long_head, short_tail), (short_head, long_tail)


def layers(own, other, a_count, weights, pick, cut):
    units = pick.shape[1]
    width, dense_units = weights[2].shape[1], weights[2].shape[0]
    extra = dense_units - units
    full = width + units
    parts = []
    slots = 0
    for block in own + other:
        if isinstance(block, tuple):
            parts += [(block[0], slots, 0, cut), (block[1], slots, cut, None)]
        else:
            parts.append((block, slots, 0, None))
        slots += 1
    rows = parts[0][0].shape[0]
    b_count = rows - a_count
    half = slots // 2
    n_blocks = len(parts)
    inputs = [p[0] for p in parts] + list(weights) + [pick]
    n_in = len(inputs)
    chunk = 1792

    def body(*refs):
        ins = refs[:n_in]
        own_ref, other_ref = refs[n_in : n_in + 2]
        gate, up, da, e_gate, e_up, db = ins[n_blocks : n_blocks + 6]
        xa, xb, a_acc, b_acc, ha, hb, sems = refs[n_in + 2 :]
        a_copies, b_copies = [], []
        for i, (_, slot, lo, hi) in enumerate(parts):
            a_cols = pl.ds(lo, (width if hi is None else hi) - lo)
            b_cols = pl.ds(lo, (full if hi is None else hi) - lo)
            from_a = ins[i].at[pl.ds(0, a_count), pl.ds(0, a_cols.size)]
            from_b = ins[i].at[pl.ds(a_count, b_count), :]
            a_copies.append(
                pltpu.make_async_copy(from_a, xa.at[pl.ds(slot * a_count, a_count), a_cols], sems.at[2 * i])
            )
            b_copies.append(
                pltpu.make_async_copy(from_b, xb.at[pl.ds(slot * b_count, b_count), b_cols], sems.at[2 * i + 1])
            )
        for c in b_copies + a_copies:
            c.start()
        a_acc[...] = jnp.zeros_like(a_acc)
        b_acc[...] = jnp.zeros_like(b_acc)
        for c in b_copies:
            c.wait()

        def b_step(i, carry):
            at = pl.ds(pl.multiple_of(i * chunk, chunk), chunk)
            w = jnp.concatenate([e_gate[at, :], e_up[at, :]], 1)
            b_acc[...] += jnp.dot(xb[:, at], w, preferred_element_type=jnp.float32)
            return carry

        lax.fori_loop(0, width // chunk, b_step, 0)
        g = b_acc[:, :units]
        value = g * (1.0 / (1.0 + jnp.exp(-g))) * b_acc[:, units:]
        tail = xb[:, width:].astype(jnp.float32) * ins[n_in - 1][...]
        hb[...] = (value * jnp.sum(tail, axis=1, keepdims=True)).astype(jnp.bfloat16)
        for c in a_copies:
            c.wait()

        def a_step(i, carry):
            at = pl.ds(pl.multiple_of(i * chunk, chunk), chunk)
            w = jnp.concatenate([gate[:units, at], up[:units, at], gate[units:, at], up[units:, at]], 0)
            a_acc[...] += lax.dot_general(
                xa[:, at], w, (((1,), (1,)), ((), ())), preferred_element_type=jnp.float32
            )
            return carry

        lax.fori_loop(0, width // chunk, a_step, 0)
        for lo, n, to in ((0, units, 0), (2 * units, extra, units)):
            g = a_acc[:, lo : lo + n]
            u = a_acc[:, lo + n : lo + 2 * n]
            ha[:, to : to + n] = (g * (1.0 / (1.0 + jnp.exp(-g))) * u).astype(jnp.bfloat16)

        def out_step(i, carry):
            at = pl.ds(pl.multiple_of(i * chunk, chunk), chunk)
            for lo, count, h, w in ((0, a_count, ha, da), (a_count, b_count, hb, db)):
                r = jnp.dot(h[...], w[:, at], preferred_element_type=jnp.float32).astype(jnp.bfloat16)
                for slot in range(slots):
                    ref = own_ref if slot < half else other_ref
                    to = pl.ds(slot % half * rows + lo, count)
                    ref[to, at] = r[slot * count : (slot + 1) * count]
            return carry

        lax.fori_loop(0, width // chunk, out_step, 0)

    hbm_spec = pl.BlockSpec(memory_space=pltpu.HBM)
    vmem_spec = pl.BlockSpec(memory_space=pltpu.VMEM)
    a_total, b_total = slots * a_count, slots * b_count
    scratch = [
        ((a_total, width), jnp.bfloat16),
        ((b_total, full), jnp.bfloat16),
        ((a_total, 2 * dense_units), jnp.float32),
        ((b_total, 2 * units), jnp.float32),
        ((a_total, dense_units), jnp.bfloat16),
        ((b_total, units), jnp.bfloat16),
    ]
    return pl.pallas_call(
        body,
        in_specs=[hbm_spec] * n_blocks + [vmem_spec] * 7,
        out_specs=[vmem_spec] * 2,
        out_shape=[jax.ShapeDtypeStruct((half * rows, width), jnp.bfloat16)] * 2,
        scratch_shapes=[pltpu.VMEM(*s) for s in scratch]
        + [pltpu.SemaphoreType.DMA((2 * n_blocks,))],
        cost_estimate=pl.CostEstimate(
            flops=6 * width * (a_total * dense_units + b_total * units),
            bytes_accessed=6 * (dense_units + units) * width + 4 * (a_total + b_total) * width,
            transcendentals=0,
        ),
        compiler_params=pltpu.CompilerParams(vmem_limit_bytes=14 * 1024 * 1024),
    )(*inputs)


def fine_size(a_rows, b_rows, a_width, b_width):
    return -(-(a_rows * a_width + b_rows * b_width) // (128 * 16)) * 16


def fine_parts(a_rows, b_rows, a_width, b_width):
    a_tiles = a_width // 128
    parts = [(t * a_rows, 0, a_rows, t) for t in range(a_tiles)]
    return parts + [
        (a_tiles * a_rows + t * b_rows, a_rows, b_rows, t) for t in range(b_width // 128)
    ]


def prepare(a_tokens, a_gain, b_tokens, b_gain, expert_ids, route_weights):
    a_rows, width = a_tokens.shape
    rows = a_rows + b_tokens.shape[0]
    lanes = 128
    full = width + lanes
    fine_rows = fine_size(a_rows, rows - a_rows, width, full)
    inputs = (a_tokens, a_gain[None], b_tokens, b_gain[None], expert_ids, route_weights)

    def body(*refs):
        out_ref, hold, fine, value = refs[6:10]
        held, sems = refs[10:16], refs[16]
        copies = [pltpu.make_async_copy(refs[i], held[i], sems.at[i]) for i in range(6)]
        for c in copies:
            c.start()
        for c in copies:
            c.wait()
        a_ref, ag_ref, b_ref, bg_ref, id_ref, w_ref = held
        hold[:a_rows, :width] = normed(a_ref[...].astype(jnp.float32), ag_ref[...])
        hold[a_rows:rows, :width] = normed(b_ref[...].astype(jnp.float32), bg_ref[...])
        lane = lax.broadcasted_iota(jnp.int32, (rows - a_rows, lanes), 1)
        expert = lane & (EXPERTS - 1)
        weight = jnp.zeros((rows - a_rows, lanes), jnp.float32)
        for k in range(expert_ids.shape[1]):
            weight += jnp.where(id_ref[:, k : k + 1] == expert, w_ref[:, k : k + 1], 0.0)
        first = weight.astype(jnp.bfloat16).astype(jnp.float32)
        second = (weight - first).astype(jnp.bfloat16).astype(jnp.float32)
        third = weight - first - second
        part = jnp.where(lane < EXPERTS, first, jnp.where(lane < 2 * EXPERTS, second, third))
        hold[a_rows:rows, width:] = jnp.where(lane < 3 * EXPERTS, part, 0.0)
        fine[pl.ds(fine_rows - 16, 16), :] = jnp.zeros((16, lanes), jnp.float32)
        for to, lo, n, t in fine_parts(a_rows, rows - a_rows, width, full):
            fine[pl.ds(to, n), :] = hold[pl.ds(lo, n), pl.ds(t * lanes, lanes)]
        value[...] = fine[...].astype(jnp.bfloat16)
        copies = [pltpu.make_async_copy(value, out_ref.at[i], sems.at[6 + i]) for i in range(RING)]
        for c in copies:
            c.start()
        for c in copies:
            c.wait()

    return pl.pallas_call(
        body,
        in_specs=[pl.BlockSpec(memory_space=pl.ANY)] * 6,
        out_specs=pl.BlockSpec(memory_space=pl.ANY),
        out_shape=jax.ShapeDtypeStruct((RING, fine_rows, lanes), jnp.bfloat16),
        scratch_shapes=[pltpu.VMEM((8, full), jnp.float32), pltpu.VMEM((fine_rows, lanes), jnp.float32)]
        + [pltpu.VMEM((fine_rows, lanes), jnp.bfloat16)]
        + [pltpu.VMEM(x.shape, x.dtype) for x in inputs]
        + [pltpu.SemaphoreType.DMA((6 + RING,))],
        compiler_params=pltpu.CompilerParams(vmem_limit_bytes=60 * 1024 * 1024),
        name="prepare",
    )(*inputs)


def pack(near, a_rows, b_rows, width):
    places, fine_rows, lanes = near.shape
    full = width + lanes
    rows = a_rows + b_rows

    def body(near_ref, out_ref, fine, hold):
        hold[pl.ds(0, places * a_rows), pl.ds(width, lanes)] = jnp.zeros(
            (places * a_rows, lanes), jnp.float32
        )
        for i in range(places):
            fine[...] = near_ref[i].astype(jnp.float32)
            for at, lo, n, t in fine_parts(a_rows, b_rows, width, full):
                to = i * a_rows if lo == 0 else places * a_rows + i * b_rows
                hold[pl.ds(to, n), pl.ds(t * lanes, lanes)] = fine[pl.ds(at, n), :]
        out_ref[...] = hold[...].astype(jnp.bfloat16)

    vmem_spec = pl.BlockSpec(memory_space=pltpu.VMEM)
    return pl.pallas_call(
        body,
        in_specs=[vmem_spec],
        out_specs=vmem_spec,
        out_shape=jax.ShapeDtypeStruct((places * rows, full), jnp.bfloat16),
        scratch_shapes=[
            pltpu.VMEM((fine_rows, lanes), jnp.float32),
            pltpu.VMEM((places * rows, full), jnp.float32),
        ],
        compiler_params=pltpu.CompilerParams(vmem_limit_bytes=6 * 1024 * 1024),
        name="pack",
    )(near)


def touch(weights, pick):
    def body(*refs):
        refs[-1][...] = refs[-2][...]

    vmem_spec = pl.BlockSpec(memory_space=pltpu.VMEM)
    return pl.pallas_call(
        body,
        in_specs=[vmem_spec] * 7,
        out_specs=vmem_spec,
        out_shape=jax.ShapeDtypeStruct(pick.shape, pick.dtype),
        compiler_params=pltpu.CompilerParams(vmem_limit_bytes=1024 * 1024),
        name="touch",
    )(*weights, pick)


def unpack(own, other, low, high, streams, a_rows):
    total, width = own.shape
    rows = total // RING
    b_rows = rows - a_rows
    count = len(streams) - 1
    lanes = 128
    fine_rows = fine_size(a_rows, b_rows, width, width)

    def body(*refs):
        own_ref, other_ref = refs[:2]
        lows, highs = refs[2 : 2 + count], refs[2 + count : 2 + 2 * count]
        out_ref, hold, one = refs[2 + 2 * count :]
        for i in range(count):
            at = slice(streams[i], streams[i + 1])
            hold[:, at] = (
                own_ref[:, at].astype(jnp.float32)
                + other_ref[:, at].astype(jnp.float32)
                + lows[i][...].astype(jnp.float32)
                + highs[i][...].astype(jnp.float32)
            )
        for j in range(RING):
            for to, lo, n, t in fine_parts(a_rows, b_rows, width, width):
                at = j * a_rows if lo == 0 else RING * a_rows + j * b_rows
                one[pl.ds(to, n), :] = hold[pl.ds(at, n), pl.ds(t * lanes, lanes)]
            out_ref[j] = one[...].astype(jnp.bfloat16)

    vmem_spec = pl.BlockSpec(memory_space=pltpu.VMEM)
    return pl.pallas_call(
        body,
        in_specs=[vmem_spec] * (2 + 2 * count),
        out_specs=vmem_spec,
        out_shape=jax.ShapeDtypeStruct((RING, fine_rows, lanes), jnp.bfloat16),
        scratch_shapes=[pltpu.VMEM((total, width), jnp.float32), pltpu.VMEM((fine_rows, lanes), jnp.float32)],
        compiler_params=pltpu.CompilerParams(vmem_limit_bytes=6 * 1024 * 1024),
        name="unpack",
    )(own, other, *low, *high)


def finish(pieces, a_tokens, b_tokens):
    a_rows, width = a_tokens.shape
    b_rows = b_tokens.shape[0]
    rows = a_rows + b_rows
    fine_rows, lanes = pieces.shape[1:]

    def body(piece_ref, a_ref, b_ref, a_out, b_out, fine, hold):
        value = piece_ref[0].astype(jnp.float32)
        for j in range(1, RING):
            value = value + piece_ref[j].astype(jnp.float32)
        fine[...] = value
        for at, lo, n, t in fine_parts(a_rows, b_rows, width, width):
            hold[pl.ds(lo, n), pl.ds(t * lanes, lanes)] = fine[pl.ds(at, n), :]
        a_out[...] = (a_ref[...].astype(jnp.float32) + hold[:a_rows]).astype(jnp.bfloat16)
        b_out[...] = (b_ref[...].astype(jnp.float32) + hold[a_rows:rows]).astype(jnp.bfloat16)

    vmem_spec = pl.BlockSpec(memory_space=pltpu.VMEM)
    return pl.pallas_call(
        body,
        in_specs=[vmem_spec] * 3,
        out_specs=[vmem_spec] * 2,
        out_shape=[
            jax.ShapeDtypeStruct(a_tokens.shape, jnp.bfloat16),
            jax.ShapeDtypeStruct(b_tokens.shape, jnp.bfloat16),
        ],
        scratch_shapes=[pltpu.VMEM((fine_rows, lanes), jnp.float32), pltpu.VMEM((8, width), jnp.float32)],
        compiler_params=pltpu.CompilerParams(vmem_limit_bytes=2 * 1024 * 1024),
        name="finish",
    )(pieces, a_tokens, b_tokens)


def shards(
    a_tokens,
    a_gain,
    dense_gate,
    dense_up,
    dense_down,
    b_tokens,
    b_gain,
    expert_ids,
    route_weights,
    expert_gate,
    expert_up,
    expert_down,
):
    devices = lax.axis_size(EXP)
    group_size = devices // EXPERTS
    width = b_tokens.shape[1]
    a_rows = a_tokens.shape[0]
    ready = prepare(a_tokens, a_gain, b_tokens, b_gain, expert_ids, route_weights)
    full = width + ready.shape[2]
    block = pack(exchange(ready), a_rows, b_tokens.shape[0], width)
    cut = width // 2
    slots = gather_ring(block, cut)
    swapped = {}
    for k, piece in slots.items():
        if isinstance(piece, tuple):
            low = swap_cores(piece[0])
            high = swap_cores(piece[1])
            swapped[k] = (low, high)
        else:
            swapped[k] = swap_cores(piece)
    expert = lax.axis_index(EXP) // group_size
    lanes = jnp.arange(full - width)
    pick = ((lanes % EXPERTS == expert) & (lanes < 3 * EXPERTS)).astype(jnp.float32)[None, :]
    weights = (
        dense_gate.T,
        dense_up.T,
        dense_down,
        expert_gate[0],
        expert_up[0],
        expert_down[0],
    )
    pick = touch(weights, pick)
    own, other = {}, {}
    rows = block.shape[0]
    for group in GROUPS:
        mine, theirs = layers(
            [slots[k] for k in group],
            [swapped[k] for k in group],
            RING * a_rows,
            weights,
            pick,
            cut,
        )
        theirs = swap_cores(theirs)
        for i, k in enumerate(group):
            own[k] = mine[i * rows : (i + 1) * rows]
            other[k] = theirs[i * rows : (i + 1) * rows]
    streams = (0, cut, width)
    low, high = scatter_ring(own, other, cut)
    pieces = unpack(own[0], other[0], low, high, streams, a_rows)
    return tuple(finish(exchange(pieces), a_tokens, b_tokens))


def solution(mesh):
    finer = Mesh(
        mesh.devices.reshape(mesh.shape["rep"], RING, RING, CORES),
        ("rep", "exp_0", "exp_1", "exp_2"),
    )
    placed = (
        P(REP_EXP, None),
        P(),
        P(None, EXP),
        P(None, EXP),
        P(EXP, None),
        P(REP_EXP, None),
        P(),
        P(REP_EXP, None),
        P(REP_EXP, None),
        P(EXP, None, None),
        P(EXP, None, None),
        P(EXP, None, None),
    )
    return jax.shard_map(
        shards,
        mesh=finer,
        in_specs=placed,
        out_specs=(P(REP_EXP, None), P(REP_EXP, None)),
        check_vma=False,
    )
```

```python
import jax
import jax.numpy as jnp
from jax import lax
from jax.experimental import pallas as pl
from jax.experimental.pallas import tpu as pltpu
from jax.sharding import Mesh
from jax.sharding import PartitionSpec as P


EXPERTS = 16
RING = 8
CORES = 2
EXP = ("exp_0", "exp_1", "exp_2")
REP_EXP = ("rep", "exp_0", "exp_1", "exp_2")


def pairs_along(stage, partner):
    pairs = []
    for x in range(RING):
        for y in range(RING):
            for c in range(CORES):
                along_x = (stage == 2) == (c == 0)
                to_x = partner(x) if along_x else x
                to_y = y if along_x else partner(y)
                pairs.append(((x * RING + y) * CORES + c, (to_x * RING + to_y) * CORES + c))
    return pairs


def even_partner(i):
    return i ^ 1


def odd_partner(i):
    return (((i + 1) % RING) ^ 1) - 1 if i else RING - 1


def over_even(array):
    return lax.ppermute(array, EXP, pairs_along(2, even_partner))


def over_odd(array):
    return lax.ppermute(array, EXP, pairs_along(2, odd_partner))


def swap_cores(array):
    devices = RING * RING * CORES
    return lax.ppermute(array, EXP, [(i, i ^ 1) for i in range(devices)])


def normed(values, gain_vec):
    return values * lax.rsqrt(jnp.mean(values * values, axis=-1, keepdims=True) + 1e-06) * gain_vec


GROUPS = ((0, 1, -1), (2, -2, 3, -3), (4,))


def stage_1_groups():
    first = [[(x * RING + y) * CORES for y in range(RING)] for x in range(RING)]
    second = [[(x * RING + y) * CORES + 1 for x in range(RING)] for y in range(RING)]
    return first + second


def exchange(blocks):
    return lax.all_to_all(
        blocks, EXP, split_axis=0, concat_axis=0, tiled=True, axis_index_groups=stage_1_groups()
    )


def gather_ring(block, cut):
    slots = {0: block}
    for k in (1, 2):
        slots[k] = over_even(slots[1 - k])
        slots[-k] = over_odd(slots[k - 1])
    even_high = over_even(slots[-2][:, cut:])
    odd_low = over_odd(slots[2][:, :cut])
    even_low = over_even(slots[-2][:, :cut])
    odd_high = over_odd(slots[2][:, cut:])
    slots[3], slots[-3] = (even_low, even_high), (odd_low, odd_high)
    low = over_even(odd_low)
    high = over_odd(even_high)
    slots[4] = (low, high)
    return slots


def scatter_ring(own, other, cut):
    width = own[0].shape[1]
    head, tail = (0, cut), (cut, width)

    def part(k, cols):
        lo, hi = cols
        return own[k][:, lo:hi].astype(jnp.float32) + other[k][:, lo:hi].astype(jnp.float32)

    def add(k, cols, piece):
        return (part(k, cols) + piece.astype(jnp.float32)).astype(jnp.bfloat16)

    short_head = over_even(part(3, head).astype(jnp.bfloat16))
    short_tail = over_odd(part(-3, tail).astype(jnp.bfloat16))
    long_head = over_even(part(4, head).astype(jnp.bfloat16))
    long_tail = over_odd(part(4, tail).astype(jnp.bfloat16))
    for step, k in enumerate((2, 1, 0)):
        side = -1 if step == 0 else 1
        even, odd = (over_odd, over_even) if step == 0 else (over_even, over_odd)
        if k:
            short = add(side * k, head, short_head), add(-side * k, tail, short_tail)
            long_head, long_tail, *_ = lax.optimization_barrier((long_head, long_tail, *short))
            short_head = even(short[0])
            short_tail = odd(short[1])
        side = 1 if step == 1 else -1
        even, odd = (over_even, over_odd) if step == 1 else (over_odd, over_even)
        long = add(side * (k + 1), head, long_head), add(-side * (k + 1), tail, long_tail)
        long_head = even(long[0])
        long_tail = odd(long[1])
    return (long_head, short_tail), (short_head, long_tail)


def layers(own, other, a_count, weights, pick, cut):
    units = pick.shape[1]
    width, dense_units = weights[2].shape[1], weights[2].shape[0]
    extra = dense_units - units
    full = width + units
    parts = []
    slots = 0
    for block in own + other:
        if isinstance(block, tuple):
            parts += [(block[0], slots, 0, cut), (block[1], slots, cut, None)]
        else:
            parts.append((block, slots, 0, None))
        slots += 1
    rows = parts[0][0].shape[0]
    b_count = rows - a_count
    half = slots // 2
    n_blocks = len(parts)
    inputs = [p[0] for p in parts] + list(weights) + [pick]
    n_in = len(inputs)
    chunk = 1792

    def body(*refs):
        ins = refs[:n_in]
        own_ref, other_ref = refs[n_in : n_in + 2]
        gate, up, da, e_gate, e_up, db = ins[n_blocks : n_blocks + 6]
        xa, xb, a_acc, b_acc, ha, hb, sems = refs[n_in + 2 :]
        a_copies, b_copies = [], []
        for i, (_, slot, lo, hi) in enumerate(parts):
            a_cols = pl.ds(lo, (width if hi is None else hi) - lo)
            b_cols = pl.ds(lo, (full if hi is None else hi) - lo)
            from_a = ins[i].at[pl.ds(0, a_count), pl.ds(0, a_cols.size)]
            from_b = ins[i].at[pl.ds(a_count, b_count), :]
            a_copies.append(
                pltpu.make_async_copy(from_a, xa.at[pl.ds(slot * a_count, a_count), a_cols], sems.at[2 * i])
            )
            b_copies.append(
                pltpu.make_async_copy(from_b, xb.at[pl.ds(slot * b_count, b_count), b_cols], sems.at[2 * i + 1])
            )
        for c in b_copies + a_copies:
            c.start()
        a_acc[...] = jnp.zeros_like(a_acc)
        b_acc[...] = jnp.zeros_like(b_acc)
        for c in b_copies:
            c.wait()

        def b_step(i, carry):
            at = pl.ds(pl.multiple_of(i * chunk, chunk), chunk)
            w = jnp.concatenate([e_gate[at, :], e_up[at, :]], 1)
            b_acc[...] += jnp.dot(xb[:, at], w, preferred_element_type=jnp.float32)
            return carry

        lax.fori_loop(0, width // chunk, b_step, 0)
        g = b_acc[:, :units]
        value = g * (1.0 / (1.0 + jnp.exp(-g))) * b_acc[:, units:]
        tail = xb[:, width:].astype(jnp.float32) * ins[n_in - 1][...]
        hb[...] = (value * jnp.sum(tail, axis=1, keepdims=True)).astype(jnp.bfloat16)
        for c in a_copies:
            c.wait()

        def a_step(i, carry):
            at = pl.ds(pl.multiple_of(i * chunk, chunk), chunk)
            w = jnp.concatenate([gate[:units, at], up[:units, at], gate[units:, at], up[units:, at]], 0)
            a_acc[...] += lax.dot_general(
                xa[:, at], w, (((1,), (1,)), ((), ())), preferred_element_type=jnp.float32
            )
            return carry

        lax.fori_loop(0, width // chunk, a_step, 0)
        for lo, n, to in ((0, units, 0), (2 * units, extra, units)):
            g = a_acc[:, lo : lo + n]
            u = a_acc[:, lo + n : lo + 2 * n]
            ha[:, to : to + n] = (g * (1.0 / (1.0 + jnp.exp(-g))) * u).astype(jnp.bfloat16)

        def out_step(i, carry):
            at = pl.ds(pl.multiple_of(i * chunk, chunk), chunk)
            for lo, count, h, w in ((0, a_count, ha, da), (a_count, b_count, hb, db)):
                r = jnp.dot(h[...], w[:, at], preferred_element_type=jnp.float32).astype(jnp.bfloat16)
                for slot in range(slots):
                    ref = own_ref if slot < half else other_ref
                    to = pl.ds(slot % half * rows + lo, count)
                    ref[to, at] = r[slot * count : (slot + 1) * count]
            return carry

        lax.fori_loop(0, width // chunk, out_step, 0)

    hbm_spec = pl.BlockSpec(memory_space=pltpu.HBM)
    vmem_spec = pl.BlockSpec(memory_space=pltpu.VMEM)
    a_total, b_total = slots * a_count, slots * b_count
    scratch = [
        ((a_total, width), jnp.bfloat16),
        ((b_total, full), jnp.bfloat16),
        ((a_total, 2 * dense_units), jnp.float32),
        ((b_total, 2 * units), jnp.float32),
        ((a_total, dense_units), jnp.bfloat16),
        ((b_total, units), jnp.bfloat16),
    ]
    return pl.pallas_call(
        body,
        in_specs=[hbm_spec] * n_blocks + [vmem_spec] * 7,
        out_specs=[vmem_spec] * 2,
        out_shape=[jax.ShapeDtypeStruct((half * rows, width), jnp.bfloat16)] * 2,
        scratch_shapes=[pltpu.VMEM(*s) for s in scratch]
        + [pltpu.SemaphoreType.DMA((2 * n_blocks,))],
        cost_estimate=pl.CostEstimate(
            flops=6 * width * (a_total * dense_units + b_total * units),
            bytes_accessed=6 * (dense_units + units) * width + 4 * (a_total + b_total) * width,
            transcendentals=0,
        ),
        compiler_params=pltpu.CompilerParams(vmem_limit_bytes=14 * 1024 * 1024),
    )(*inputs)


def fine_size(a_rows, b_rows, a_width, b_width):
    return -(-(a_rows * a_width + b_rows * b_width) // (128 * 16)) * 16


def fine_parts(a_rows, b_rows, a_width, b_width):
    a_tiles = a_width // 128
    parts = [(t * a_rows, 0, a_rows, t) for t in range(a_tiles)]
    return parts + [
        (a_tiles * a_rows + t * b_rows, a_rows, b_rows, t) for t in range(b_width // 128)
    ]


def prepare(a_tokens, a_gain, b_tokens, b_gain, expert_ids, route_weights):
    a_rows, width = a_tokens.shape
    rows = a_rows + b_tokens.shape[0]
    lanes = 128
    full = width + lanes
    fine_rows = fine_size(a_rows, rows - a_rows, width, full)
    inputs = (a_tokens, a_gain[None], b_tokens, b_gain[None], expert_ids, route_weights)

    def body(*refs):
        out_ref, hold, fine, value = refs[6:10]
        held, sems = refs[10:16], refs[16]
        copies = [pltpu.make_async_copy(refs[i], held[i], sems.at[i]) for i in range(6)]
        for c in copies:
            c.start()
        for c in copies:
            c.wait()
        a_ref, ag_ref, b_ref, bg_ref, id_ref, w_ref = held
        hold[:a_rows, :width] = normed(a_ref[...].astype(jnp.float32), ag_ref[...])
        hold[a_rows:rows, :width] = normed(b_ref[...].astype(jnp.float32), bg_ref[...])
        lane = lax.broadcasted_iota(jnp.int32, (rows - a_rows, lanes), 1)
        expert = lane & (EXPERTS - 1)
        weight = jnp.zeros((rows - a_rows, lanes), jnp.float32)
        for k in range(expert_ids.shape[1]):
            weight += jnp.where(id_ref[:, k : k + 1] == expert, w_ref[:, k : k + 1], 0.0)
        first = weight.astype(jnp.bfloat16).astype(jnp.float32)
        second = (weight - first).astype(jnp.bfloat16).astype(jnp.float32)
        third = weight - first - second
        part = jnp.where(lane < EXPERTS, first, jnp.where(lane < 2 * EXPERTS, second, third))
        hold[a_rows:rows, width:] = jnp.where(lane < 3 * EXPERTS, part, 0.0)
        fine[pl.ds(fine_rows - 16, 16), :] = jnp.zeros((16, lanes), jnp.float32)
        for to, lo, n, t in fine_parts(a_rows, rows - a_rows, width, full):
            fine[pl.ds(to, n), :] = hold[pl.ds(lo, n), pl.ds(t * lanes, lanes)]
        value[...] = fine[...].astype(jnp.bfloat16)
        copies = [pltpu.make_async_copy(value, out_ref.at[i], sems.at[6 + i]) for i in range(RING)]
        for c in copies:
            c.start()
        for c in copies:
            c.wait()

    return pl.pallas_call(
        body,
        in_specs=[pl.BlockSpec(memory_space=pl.ANY)] * 6,
        out_specs=pl.BlockSpec(memory_space=pl.ANY),
        out_shape=jax.ShapeDtypeStruct((RING, fine_rows, lanes), jnp.bfloat16),
        scratch_shapes=[pltpu.VMEM((8, full), jnp.float32), pltpu.VMEM((fine_rows, lanes), jnp.float32)]
        + [pltpu.VMEM((fine_rows, lanes), jnp.bfloat16)]
        + [pltpu.VMEM(x.shape, x.dtype) for x in inputs]
        + [pltpu.SemaphoreType.DMA((6 + RING,))],
        compiler_params=pltpu.CompilerParams(vmem_limit_bytes=60 * 1024 * 1024),
        name="prepare",
    )(*inputs)


def pack(near, a_rows, b_rows, width):
    places, fine_rows, lanes = near.shape
    full = width + lanes
    rows = a_rows + b_rows

    def body(near_ref, out_ref, fine, hold):
        hold[pl.ds(0, places * a_rows), pl.ds(width, lanes)] = jnp.zeros(
            (places * a_rows, lanes), jnp.float32
        )
        for i in range(places):
            fine[...] = near_ref[i].astype(jnp.float32)
            for at, lo, n, t in fine_parts(a_rows, b_rows, width, full):
                to = i * a_rows if lo == 0 else places * a_rows + i * b_rows
                hold[pl.ds(to, n), pl.ds(t * lanes, lanes)] = fine[pl.ds(at, n), :]
        out_ref[...] = hold[...].astype(jnp.bfloat16)

    vmem_spec = pl.BlockSpec(memory_space=pltpu.VMEM)
    return pl.pallas_call(
        body,
        in_specs=[vmem_spec],
        out_specs=vmem_spec,
        out_shape=jax.ShapeDtypeStruct((places * rows, full), jnp.bfloat16),
        scratch_shapes=[
            pltpu.VMEM((fine_rows, lanes), jnp.float32),
            pltpu.VMEM((places * rows, full), jnp.float32),
        ],
        compiler_params=pltpu.CompilerParams(vmem_limit_bytes=6 * 1024 * 1024),
        name="pack",
    )(near)


def touch(weights, pick):
    def body(*refs):
        refs[-1][...] = refs[-2][...]

    vmem_spec = pl.BlockSpec(memory_space=pltpu.VMEM)
    return pl.pallas_call(
        body,
        in_specs=[vmem_spec] * 7,
        out_specs=vmem_spec,
        out_shape=jax.ShapeDtypeStruct(pick.shape, pick.dtype),
        compiler_params=pltpu.CompilerParams(vmem_limit_bytes=1024 * 1024),
        name="touch",
    )(*weights, pick)


def unpack(own, other, low, high, streams, a_rows):
    total, width = own.shape
    rows = total // RING
    b_rows = rows - a_rows
    count = len(streams) - 1
    lanes = 128
    fine_rows = fine_size(a_rows, b_rows, width, width)

    def body(*refs):
        own_ref, other_ref = refs[:2]
        lows, highs = refs[2 : 2 + count], refs[2 + count : 2 + 2 * count]
        out_ref, hold, one = refs[2 + 2 * count :]
        for i in range(count):
            at = slice(streams[i], streams[i + 1])
            hold[:, at] = (
                own_ref[:, at].astype(jnp.float32)
                + other_ref[:, at].astype(jnp.float32)
                + lows[i][...].astype(jnp.float32)
                + highs[i][...].astype(jnp.float32)
            )
        for j in range(RING):
            for to, lo, n, t in fine_parts(a_rows, b_rows, width, width):
                at = j * a_rows if lo == 0 else RING * a_rows + j * b_rows
                one[pl.ds(to, n), :] = hold[pl.ds(at, n), pl.ds(t * lanes, lanes)]
            out_ref[j] = one[...].astype(jnp.bfloat16)

    vmem_spec = pl.BlockSpec(memory_space=pltpu.VMEM)
    return pl.pallas_call(
        body,
        in_specs=[vmem_spec] * (2 + 2 * count),
        out_specs=vmem_spec,
        out_shape=jax.ShapeDtypeStruct((RING, fine_rows, lanes), jnp.bfloat16),
        scratch_shapes=[pltpu.VMEM((total, width), jnp.float32), pltpu.VMEM((fine_rows, lanes), jnp.float32)],
        compiler_params=pltpu.CompilerParams(vmem_limit_bytes=6 * 1024 * 1024),
        name="unpack",
    )(own, other, *low, *high)


def finish(pieces, a_tokens, b_tokens):
    a_rows, width = a_tokens.shape
    b_rows = b_tokens.shape[0]
    rows = a_rows + b_rows
    fine_rows, lanes = pieces.shape[1:]

    def body(piece_ref, a_ref, b_ref, a_out, b_out, fine, hold):
        value = piece_ref[0].astype(jnp.float32)
        for j in range(1, RING):
            value = value + piece_ref[j].astype(jnp.float32)
        fine[...] = value
        for at, lo, n, t in fine_parts(a_rows, b_rows, width, width):
            hold[pl.ds(lo, n), pl.ds(t * lanes, lanes)] = fine[pl.ds(at, n), :]
        a_out[...] = (a_ref[...].astype(jnp.float32) + hold[:a_rows]).astype(jnp.bfloat16)
        b_out[...] = (b_ref[...].astype(jnp.float32) + hold[a_rows:rows]).astype(jnp.bfloat16)

    vmem_spec = pl.BlockSpec(memory_space=pltpu.VMEM)
    return pl.pallas_call(
        body,
        in_specs=[vmem_spec] * 3,
        out_specs=[vmem_spec] * 2,
        out_shape=[
            jax.ShapeDtypeStruct(a_tokens.shape, jnp.bfloat16),
            jax.ShapeDtypeStruct(b_tokens.shape, jnp.bfloat16),
        ],
        scratch_shapes=[pltpu.VMEM((fine_rows, lanes), jnp.float32), pltpu.VMEM((8, width), jnp.float32)],
        compiler_params=pltpu.CompilerParams(vmem_limit_bytes=2 * 1024 * 1024),
        name="finish",
    )(pieces, a_tokens, b_tokens)


def shards(
    a_tokens,
    a_gain,
    dense_gate,
    dense_up,
    dense_down,
    b_tokens,
    b_gain,
    expert_ids,
    route_weights,
    expert_gate,
    expert_up,
    expert_down,
):
    devices = lax.axis_size(EXP)
    group_size = devices // EXPERTS
    width = b_tokens.shape[1]
    a_rows = a_tokens.shape[0]
    ready = prepare(a_tokens, a_gain, b_tokens, b_gain, expert_ids, route_weights)
    full = width + ready.shape[2]
    block = pack(exchange(ready), a_rows, b_tokens.shape[0], width)
    cut = width // 2
    slots = gather_ring(block, cut)
    swapped = {}
    for k, piece in slots.items():
        if isinstance(piece, tuple):
            low = swap_cores(piece[0])
            high = swap_cores(piece[1])
            swapped[k] = (low, high)
        else:
            swapped[k] = swap_cores(piece)
    expert = lax.axis_index(EXP) // group_size
    lanes = jnp.arange(full - width)
    pick = ((lanes % EXPERTS == expert) & (lanes < 3 * EXPERTS)).astype(jnp.float32)[None, :]
    weights = (
        dense_gate.T,
        dense_up.T,
        dense_down,
        expert_gate[0],
        expert_up[0],
        expert_down[0],
    )
    pick = touch(weights, pick)
    own, other = {}, {}
    rows = block.shape[0]
    for group in GROUPS:
        mine, theirs = layers(
            [slots[k] for k in group],
            [swapped[k] for k in group],
            RING * a_rows,
            weights,
            pick,
            cut,
        )
        theirs = swap_cores(theirs)
        for i, k in enumerate(group):
            own[k] = mine[i * rows : (i + 1) * rows]
            other[k] = theirs[i * rows : (i + 1) * rows]
    streams = (0, cut, width)
    low, high = scatter_ring(own, other, cut)
    pieces = unpack(own[0], other[0], low, high, streams, a_rows)
    return tuple(finish(exchange(pieces), a_tokens, b_tokens))


def solution(mesh):
    finer = Mesh(
        mesh.devices.reshape(mesh.shape["rep"], RING, RING, CORES),
        ("rep", "exp_0", "exp_1", "exp_2"),
    )
    placed = (
        P(REP_EXP, None),
        P(),
        P(None, EXP),
        P(None, EXP),
        P(EXP, None),
        P(REP_EXP, None),
        P(),
        P(REP_EXP, None),
        P(REP_EXP, None),
        P(EXP, None, None),
        P(EXP, None, None),
        P(EXP, None, None),
    )
    return jax.shard_map(
        shards,
        mesh=finer,
        in_specs=placed,
        out_specs=(P(REP_EXP, None), P(REP_EXP, None)),
        check_vma=False,
    )
```
